32 devices in a mesh: groups: 2 (over y), seq: 4 (over x, core), tensor: 4 (over z).
Axes of the slice: x: 2, y: 2, z: 4, core: 2. Of those that a mesh axis runs over, the one named last changes fastest.
Arguments:
- hidden: bfloat16 [256, 4608], P(('groups', 'seq')), parts along dimension 0, may hold values from -6 to 6
- pre_gain: float32 [4608], replicated, may hold values from 0.25 to 1.75
- w_query: bfloat16 [4608, 4096], P(None, 'tensor'), may hold values from -0.09375 to 0.09375
- w_key: bfloat16 [4608, 2048], P(None, 'tensor'), may hold values from -0.09375 to 0.09375
- w_value: bfloat16 [4608, 2048], P(None, 'tensor'), may hold values from -0.09375 to 0.09375
- w_out: bfloat16 [4096, 4608], P('tensor'), may hold values from -0.125 to 0.125
- post_gain: float32 [4608], P('tensor'), may hold values from 0.25 to 1.75
- cache_pool: bfloat16 [512, 2, 128, 2048], P(('groups', 'seq'), None, None, 'tensor'), parts along dimension 0, may hold values from -6 to 6
- prompt_cache: bfloat16 [256, 2, 64, 2048], P('seq', None, None, 'tensor'), may hold values from -6 to 6
- task_ids: int32 [256], P('groups'), parts along dimension 0, may hold values from 0 to 255
- cache_lengths: int32 [256], P('groups'), parts along dimension 0, may hold values from 1 to 4096, as said below
- block_table: int32 [256, 32], P('groups'), parts along dimension 0, may hold values from -1 to 255, as said below
Outputs:
- layer_out: bfloat16 [256, 4608], P(('groups', 'seq'), 'tensor'), parts along dimension 0
- fresh_cache: bfloat16 [256, 2, 2048], P(('groups', 'seq'), None, 'tensor'), parts along dimension 0
The draws below stay inside these ranges and needn't reach their ends.
There are 2 independent parts, one for each index of `groups`. The reference program is written for one: setup_inputs(seed, part) draws one part's arguments, and reference() takes and returns one part's arrays. A program takes and returns all parts, laid end to end along the dimension named above; an argument that names none is the same for every part. Nothing has to cross between parts.
Inputs may be any that keep to these rules, and one draw needn't show every extreme that they name: `cache_lengths`: each draw has a request with exactly 4096 cache tokens. block_table[r, j] is the page of cache_pool holding cache tokens j * 128 to (j + 1) * 128 - 1 of request r for j < ceil(cache_lengths[r] / 128), and -1 for the later j; no page is named twice.
All inputs are finite; a program needn't handle non-finite values.
Results may differ from the reference program's by a relative error of at most 0.018.
Values may be sent and summed in bfloat16 or wider, within the bound.
A program may use at most 128 MiB of HBM per device.

```python
import math
import jax
import jax.numpy as jnp
import numpy as np
from jax import lax

D = 4608
H = 32
KVH = 16
HD = 128
BLOCK = 128
PROMPT = 64
MAXLEN = 4096
MAXBLK = 32
TASKS = 256
REQ = 128
POOL = 256


def lengths_and_blocks(key):
    base = jax.random.fold_in(key, 7)
    k_first, k_second, k_order, k_tail, k_large, k_pages = jax.random.split(base, 6)
    extra = POOL - REQ - MAXBLK
    first_pick = jax.random.randint(k_first, (extra,), 0, REQ)
    second_pick = jax.random.randint(k_second, (extra,), 0, REQ)
    skewed = first_pick * second_pick // REQ
    order = jax.random.permutation(k_order, REQ)
    picked = order[skewed]
    counts = jnp.sum((picked[:, None] == jnp.arange(REQ)[None, :]).astype(jnp.int32), axis=0)
    largest = jax.random.randint(k_large, (), 0, REQ)
    is_large = jnp.arange(REQ) == largest
    blocks = jnp.where(is_large, MAXBLK, jnp.minimum(1 + counts, MAXBLK)).astype(jnp.int32)
    tails = jax.random.randint(k_tail, (REQ,), 1, BLOCK + 1)
    lengths = jnp.where(is_large, MAXLEN, (blocks - 1) * BLOCK + tails)
    offsets = jnp.cumsum(blocks) - blocks
    pages = jax.random.permutation(k_pages, POOL)
    slots = offsets[:, None] + jnp.arange(MAXBLK)[None, :]
    live_slot = jnp.arange(MAXBLK)[None, :] < blocks[:, None]
    table = jnp.where(live_slot, pages[jnp.minimum(slots, POOL - 1)], -1)
    return (lengths.astype(jnp.int32), table.astype(jnp.int32))


def draw_cache_lengths(key, part):
    return lengths_and_blocks(key)[0]


def draw_block_table(key, part):
    return lengths_and_blocks(key)[1]


def place_ends(values, own_key, least, high):
    longest = values.shape.index(max(values.shape))
    spots = []
    for shift in (0, 1):
        where = [jax.random.randint(jax.random.fold_in(own_key, axis), (), 0, length) for axis, length in enumerate(values.shape)]
        where[longest] = (where[longest] + shift) % values.shape[longest]
        spots.append(tuple(where))
    return values.at[spots[0]].set(least).at[spots[1]].set(high)


def spiked(drawn, stream_key, source, target, shards_of, factor):
    owner, partner = [(jnp.arange(drawn.shape[dim]) // (drawn.shape[dim] // shards_of)).reshape([-1 if axis == dim else 1 for axis in range(drawn.ndim)]) for dim in (source, target)]
    chosen = jax.random.permutation(stream_key, shards_of)[partner]
    strong = (owner == chosen) | (owner == (partner + shards_of // 2) % shards_of)
    return jnp.where(strong, factor * drawn, drawn)


def shard_levels(own_key, dims, pieces, low, high):
    loudness = 1.0
    for dim, shards_of in pieces:
        draws = jax.random.uniform(jax.random.fold_in(jax.random.fold_in(own_key, 6), dim), (shards_of,), jnp.float32, low / len(pieces), high / len(pieces))
        loudness = loudness * jnp.repeat(jnp.exp(draws), dims[dim] // shards_of).reshape((-1,) + (1,) * (len(dims) - 1 - dim))
    return loudness


def cumulative_ranks(amount, skew):
    portions = [(1 << 20) // math.isqrt(rank ** skew) + 1 for rank in range(1, amount + 1)]
    spread = 1 + sum(portions) // (1 << 30)
    return np.cumsum(np.array([max(1, weight // spread) for weight in portions]))


def skewed_ids(stream_key, dims, count, lean):
    grid = cumulative_ranks(count, lean)
    ticket = jax.random.randint(jax.random.fold_in(stream_key, 1), dims, 0, int(grid[count - 1]))
    grade = jnp.searchsorted(jnp.asarray(grid, jnp.int32), ticket, side="right")
    return jax.random.permutation(jax.random.fold_in(stream_key, 2), count)[grade].astype(jnp.int32)


def bell_draw(key, extent, scale, most, cuts=(), kind=jnp.bfloat16):
    level = shard_levels(key, extent, cuts, -0.22, 0.18) if cuts else 1.0
    values = jax.random.normal(key, extent, jnp.float32) * scale * level
    return jnp.minimum(jnp.maximum(values, -most), most).astype(kind)


def heavy_noise(stream_key, extent, spread, bound, pieces, heavy, kind=jnp.bfloat16):
    array = spread * jax.random.normal(stream_key, extent, jnp.float32)
    if pieces:
        array = array * shard_levels(stream_key, extent, pieces, -0.22, 0.18)
    return jnp.clip(spiked(array, jax.random.fold_in(stream_key, 3), *heavy), -bound, bound).astype(kind)


def setup_inputs(seed: int = 0, part: int = 0) -> dict:
    key_list = jax.random.split(jax.random.key(seed), 13)
    part_keys = jax.random.split(jax.random.fold_in(key_list[12], part), 13)
    hidden = bell_draw(part_keys[0], (REQ, D), 1.0, 6.0, ((0, 4),))
    pre_gain = jnp.clip(1.0 + 0.15 * jax.random.normal(key_list[1], (D,), jnp.float32), 0.25, 1.75)
    w_query = bell_draw(key_list[2], (D, H * HD), D ** -0.5, 0.09375, ((1, 4),))
    w_key = bell_draw(key_list[3], (D, KVH * HD), D ** -0.5, 0.09375, ((1, 4),))
    w_value = bell_draw(key_list[4], (D, KVH * HD), D ** -0.5, 0.09375, ((1, 4),))
    w_out = heavy_noise(key_list[5], (H * HD, D), (H * HD) ** -0.5, 0.125, ((0, 4),), (0, 1, 4, 2.0))
    post_gain = jnp.clip(1.0 + 0.15 * jax.random.normal(key_list[6], (D,), jnp.float32), 0.25, 1.75)
    cache_pool = bell_draw(part_keys[7], (POOL, 2, BLOCK, KVH * HD), 1.0, 6.0, ((0, 4), (3, 4)))
    prompt_cache = bell_draw(key_list[8], (TASKS, 2, PROMPT, KVH * HD), 1.0, 6.0, ((0, 4), (3, 4)))
    task_ids = place_ends(skewed_ids(part_keys[9], (REQ,), TASKS, 2), jax.random.fold_in(part_keys[9], 3), 0, TASKS - 1).astype(jnp.int32)
    cache_lengths = draw_cache_lengths(jax.random.fold_in(jax.random.fold_in(key_list[12], part), 71), part)
    block_table = draw_block_table(jax.random.fold_in(jax.random.fold_in(key_list[12], part), 71), part)
    return dict(hidden=hidden, pre_gain=pre_gain, w_query=w_query, w_key=w_key, w_value=w_value, w_out=w_out, post_gain=post_gain, cache_pool=cache_pool, prompt_cache=prompt_cache, task_ids=task_ids, cache_lengths=cache_lengths, block_table=block_table)


cap_limit = 50.0

def rms_scale(values, gain):
    mean_square = lax.optimization_barrier(jnp.mean(values * values, axis=-1, keepdims=True))
    return values * lax.rsqrt(mean_square + 1e-06) * gain

def rotate(values, position):
    half_dim = values.shape[-1] // 2
    frequency = 10000.0 ** (-jnp.arange(half_dim, dtype=jnp.float32) / half_dim)
    angles = position.astype(jnp.float32)[:, None] * frequency[None, :]
    cosine = jnp.cos(angles)[:, None, :]
    sines = jnp.sin(angles)[:, None, :]
    first_half = values[..., :half_dim]
    second_half = values[..., half_dim:]
    return jnp.concatenate([first_half * cosine - second_half * sines, second_half * cosine + first_half * sines], axis=-1)

def capped(raw_score, score_scale):
    return cap_limit * jnp.tanh(raw_score * score_scale / cap_limit)

def reference(hidden, pre_gain, w_query, w_key, w_value, w_out, post_gain, cache_pool, prompt_cache, task_ids, cache_lengths, block_table):
    normed = rms_scale(hidden.astype(jnp.float32), pre_gain.astype(jnp.float32)).astype(jnp.bfloat16)
    position = (PROMPT + cache_lengths).astype(jnp.int32)
    query_rows = rotate(jnp.dot(normed, w_query, preferred_element_type=jnp.float32).reshape(REQ, H, HD), position).astype(jnp.bfloat16)
    key_new = rotate(jnp.dot(normed, w_key, preferred_element_type=jnp.float32).reshape(REQ, KVH, HD), position).astype(jnp.bfloat16)
    value_new = jnp.dot(normed, w_value, preferred_element_type=jnp.float32).astype(jnp.bfloat16)
    fresh_cache = jnp.stack([key_new.reshape(REQ, KVH * HD), value_new], axis=1)
    score_scale = float(D // H) ** (-0.5)
    group_size = H // KVH

    def one_request(request_args):
        query_one, task_one, length_one, row_one, key_one, value_one = request_args
        request_pages = cache_pool[jnp.maximum(row_one, 0)]
        cache_keys = request_pages[:, 0].reshape(MAXBLK * BLOCK, KVH, HD)
        cache_values = request_pages[:, 1].reshape(MAXBLK * BLOCK, KVH, HD)
        prompt = prompt_cache[task_one]
        all_keys = jnp.concatenate([prompt[0].reshape(PROMPT, KVH, HD), cache_keys, key_one[None]], axis=0)
        all_values = jnp.concatenate([prompt[1].reshape(PROMPT, KVH, HD), cache_values, value_one.reshape(1, KVH, HD)], axis=0)
        key_mask = jnp.concatenate([jnp.ones((PROMPT,), bool), jnp.arange(MAXBLK * BLOCK) < length_one, jnp.ones((1,), bool)])
        grouped = query_one.reshape(KVH, group_size, HD).astype(jnp.float32)
        raw_score = jnp.einsum('kgd,tkd->kgt', grouped, all_keys.astype(jnp.float32))
        weight = jnp.where(key_mask[None, None, :], jnp.exp(capped(raw_score, score_scale)), 0.0)
        weight_sum = lax.optimization_barrier(jnp.sum(weight, axis=-1))
        rounded = lax.optimization_barrier(weight.astype(jnp.bfloat16)).astype(jnp.float32)
        mixture = jnp.einsum('kgt,tkd->kgd', rounded, all_values.astype(jnp.float32))
        return (mixture / weight_sum[..., None]).reshape(H * HD).astype(jnp.bfloat16)
    attended = lax.map(one_request, (query_rows, task_ids, cache_lengths, block_table, key_new, value_new))
    projected = jnp.dot(attended, w_out, preferred_element_type=jnp.float32)
    layer_out = hidden.astype(jnp.float32) + rms_scale(projected, post_gain.astype(jnp.float32))
    return (layer_out.astype(jnp.bfloat16), fresh_cache)
```

```python
import jax
import jax.numpy as jnp
from jax import lax
from jax.experimental import pallas as pl
from jax.experimental.pallas import tpu as pltpu
from jax.sharding import PartitionSpec as P
import functools
import numpy as np

D = 4608
H = 32
HD = 128


cap_limit = 50.0


def rms_scale(values, gain):
    mean_square = jnp.mean(values * values, axis=-1, keepdims=True)
    return values * lax.rsqrt(mean_square + 1e-06) * gain


def rotate(values, position):
    half_dim = values.shape[-1] // 2
    frequency = 10000.0 ** (-jnp.arange(half_dim, dtype=jnp.float32) / half_dim)
    angles = position.astype(jnp.float32)[:, None] * frequency[None, :]
    cosine = jnp.cos(angles)[:, None, :]
    sines = jnp.sin(angles)[:, None, :]
    first_half = values[..., :half_dim]
    second_half = values[..., half_dim:]
    return jnp.concatenate(
        [first_half * cosine - second_half * sines, second_half * cosine + first_half * sines],
        axis=-1,
    )


def capped(raw_score, score_scale):
    return cap_limit * jnp.tanh(raw_score * score_scale / cap_limit)


def attend(query_block, block, live_mask, score_scale):
    count = block.shape[0]
    length = block.shape[2]
    kv_heads = query_block.shape[1]
    head_dim = query_block.shape[3]
    block_keys = block[:, 0].reshape(count, length, kv_heads, head_dim)
    block_values = block[:, 1].reshape(count, length, kv_heads, head_dim)
    raw_score = jnp.einsum(
        "nkgd,ntkd->nkgt", query_block, block_keys, preferred_element_type=jnp.float32
    )
    weight = jnp.where(live_mask[:, None, None, :], jnp.exp(capped(raw_score, score_scale)), 0.0)
    totals = jnp.sum(weight, axis=-1).reshape(count, -1)
    mixtures = jnp.einsum(
        "nkgt,ntkd->nkgd",
        weight.astype(jnp.bfloat16),
        block_values,
        preferred_element_type=jnp.float32,
    )
    return (totals, mixtures.reshape(count, -1))


def plain_body(
    hidden,
    pre_gain,
    w_query,
    w_key,
    w_value,
    w_out,
    post_gain,
    cache_pool,
    prompt_cache,
    task_ids,
    cache_lengths,
    block_table,
):
    seq_index = lax.axis_index("seq")
    tensor_index = lax.axis_index("tensor")
    own_rows = hidden.shape[0]
    requests = task_ids.shape[0]
    pages_dev = cache_pool.shape[0]
    block_len = cache_pool.shape[2]
    kv_width = cache_pool.shape[3]
    head_dim = HD
    kv_heads = kv_width // head_dim
    query_heads = w_query.shape[1] // head_dim
    group_size = query_heads // kv_heads
    prompt_len = prompt_cache.shape[2]
    tasks_dev = prompt_cache.shape[0]
    score_scale = float(D // H) ** (-0.5)
    first_row = seq_index * own_rows
    own_lengths = lax.dynamic_slice_in_dim(cache_lengths, first_row, own_rows)
    normed = rms_scale(hidden.astype(jnp.float32), pre_gain).astype(jnp.bfloat16)
    position = prompt_len + own_lengths
    query_rows = rotate(
        jnp.dot(normed, w_query, preferred_element_type=jnp.float32).reshape(
            own_rows, query_heads, head_dim
        ),
        position,
    ).astype(jnp.bfloat16)
    key_new = rotate(
        jnp.dot(normed, w_key, preferred_element_type=jnp.float32).reshape(
            own_rows, kv_heads, head_dim
        ),
        position,
    ).astype(jnp.bfloat16)
    value_new = jnp.dot(normed, w_value, preferred_element_type=jnp.float32).astype(jnp.bfloat16)
    fresh_cache = jnp.stack([key_new.reshape(own_rows, kv_width), value_new], axis=1)
    queries = lax.all_gather(
        query_rows.reshape(own_rows, query_heads * head_dim), "seq", axis=0, tiled=True
    )
    page_ids = seq_index * pages_dev + jnp.arange(pages_dev)
    flat_table = block_table.reshape(-1)
    max_blocks = block_table.shape[1]
    matches = flat_table[None, :] == page_ids[:, None]
    entry_index = jnp.arange(flat_table.shape[0])
    page_used = jnp.any(matches, axis=1)
    found_entry = jnp.sum(jnp.where(matches, entry_index[None, :], 0), axis=1)
    page_owner = found_entry // max_blocks
    block_number = found_entry % max_blocks
    owner_hot = (page_owner[:, None] == jnp.arange(requests)[None, :]) & page_used[:, None]
    owner_length = jnp.sum(jnp.where(owner_hot, cache_lengths[None, :], 0), axis=1)
    valid_count = jnp.clip(owner_length - block_number * block_len, 0, block_len)
    page_query = jnp.dot(
        owner_hot.astype(jnp.bfloat16), queries, preferred_element_type=jnp.float32
    ).astype(jnp.bfloat16)
    page_query = page_query.reshape(pages_dev, kv_heads, group_size, head_dim)
    page_live = jnp.arange(block_len)[None, :] < valid_count[:, None]
    page_totals, page_mixtures = attend(page_query, cache_pool, page_live, score_scale)
    spread_hot = owner_hot.astype(jnp.float32).T
    totals = jnp.dot(spread_hot, page_totals, precision=lax.Precision.HIGHEST)
    mixtures = jnp.dot(spread_hot, page_mixtures, precision=lax.Precision.HIGHEST)
    local_task = task_ids - seq_index * tasks_dev
    is_owned = (local_task >= 0) & (local_task < tasks_dev)
    task_rows = prompt_cache[jnp.clip(local_task, 0, tasks_dev - 1)]
    all_query = queries.reshape(requests, kv_heads, group_size, head_dim)
    owned_live = jnp.broadcast_to(is_owned[:, None], (requests, prompt_len))
    prompt_totals, prompt_mixtures = attend(all_query, task_rows, owned_live, score_scale)
    totals = totals + prompt_totals
    mixtures = mixtures + prompt_mixtures
    totals, mixtures = (
        lax.psum_scatter(
            totals.astype(jnp.bfloat16), "seq", scatter_dimension=0, tiled=True
        ).astype(jnp.float32),
        lax.psum_scatter(
            mixtures.astype(jnp.bfloat16), "seq", scatter_dimension=0, tiled=True
        ).astype(jnp.float32),
    )
    own_query = query_rows.reshape(own_rows, kv_heads, group_size, head_dim)
    self_raw = jnp.sum(
        own_query.astype(jnp.float32) * key_new[:, :, None, :].astype(jnp.float32), axis=-1
    )
    self_weight = jnp.exp(capped(self_raw, score_scale))
    rounded = lax.optimization_barrier(self_weight.astype(jnp.bfloat16)).astype(jnp.float32)
    totals = totals + self_weight.reshape(own_rows, -1)
    self_mix = rounded[..., None] * value_new.reshape(own_rows, kv_heads, 1, head_dim).astype(
        jnp.float32
    )
    mixtures = mixtures + self_mix.reshape(own_rows, -1)
    attended = (mixtures.reshape(own_rows, query_heads, head_dim) / totals[..., None]).astype(
        jnp.bfloat16
    )
    projected = jnp.dot(
        attended.reshape(own_rows, query_heads * head_dim),
        w_out,
        preferred_element_type=jnp.float32,
    )
    cols_local = post_gain.shape[0]
    col_start = tensor_index * cols_local
    residual = lax.dynamic_slice_in_dim(hidden, col_start, cols_local, 1).astype(jnp.float32)
    whole_sum = lax.psum(projected.astype(jnp.bfloat16), "tensor").astype(jnp.float32)
    mean_square = jnp.mean(whole_sum * whole_sum, axis=1, keepdims=True)
    scaled = lax.dynamic_slice_in_dim(whole_sum, col_start, cols_local, 1) * lax.rsqrt(
        mean_square + 1e-06
    )
    layer_out = (residual + scaled * post_gain).astype(jnp.bfloat16)
    return (layer_out, fresh_cache)


MESH = pl.DeviceIdType.MESH
VMEM_BYTES = 62 * 1024 * 1024


def rope_lanes(x, cosine, sines):
    return x * cosine + pltpu.roll(x, x.shape[-1] // 2, 1) * sines


SLOTS = 16
TOKENS = 128


def attend_groups(groups, heads, kv_heads, hd, score_scale):
    tiles = kv_heads * hd // 256
    tile_heads = heads // tiles
    rows = tile_heads * SLOTS
    slot = lax.broadcasted_iota(jnp.int32, (SLOTS, TOKENS), 0)

    def stacked(x):
        return jnp.concatenate([x] * tile_heads, axis=0)

    scores = []
    for qwide, keys, values, pairs, per, live in groups:
        unit = stacked(slot // per)
        chosen = [None] * tiles
        for pair in range(pairs):
            for t in range(tiles):
                raw = lax.dot_general(
                    qwide[t * rows : (t + 1) * rows, t * 256 : (t + 1) * 256],
                    keys(pair, t),
                    (((1,), (1,)), ((), ())),
                    preferred_element_type=jnp.float32,
                )
                for u in range(2):
                    part = raw[:, u * TOKENS : (u + 1) * TOKENS]
                    if chosen[t] is None:
                        chosen[t] = part
                    else:
                        chosen[t] = jnp.where(unit == 2 * pair + u, part, chosen[t])
        scores.append(chosen)
    results = []
    for chosen, (qwide, keys, values, pairs, per, live) in zip(scores, groups):
        wide_live = stacked(live)
        mixes, totals = [], []
        for t in range(tiles):
            weight = jnp.exp(cap_limit * jnp.tanh(chosen[t] * (score_scale / cap_limit)))
            weight = jnp.where(wide_live > 0, weight, 0.0)
            total = jnp.sum(weight, axis=1, keepdims=True)
            narrow = weight.astype(jnp.bfloat16)
            acc = None
            for pair in range(pairs):
                pieces = []
                for u in range(2):
                    keep = (slot // per == 2 * pair + u).astype(jnp.float32).astype(jnp.bfloat16)
                    pieces.append(narrow * stacked(keep))
                term = jnp.dot(
                    jnp.concatenate(pieces, axis=1),
                    values(pair, t),
                    preferred_element_type=jnp.float32,
                )
                acc = term if acc is None else acc + term
            group = heads // kv_heads
            for i in range(tile_heads):
                span = slice(i * SLOTS, (i + 1) * SLOTS)
                kv = i // group
                mixes.append(acc[span, kv * hd : (kv + 1) * hd])
                totals.append(total[span])
        lane = lax.broadcasted_iota(jnp.int32, (SLOTS, hd), 1)
        packed_total = jnp.zeros((SLOTS, hd), jnp.float32)
        for h in range(heads):
            packed_total = jnp.where(lane == h, totals[h], packed_total)
        results.append(mixes + [packed_total])
    return results


def layer_kernel(
    seq, tensor, score_scale, hd, steps,
    lengths_in, tasks_in, tasks_row_in, table_in, hidden_in, pre_gain_in, frequency_in, post_gain_in,
    w_query, w_key, w_value, w_out, pool, prompts,
    out, fresh_out,
    lengths, tasks, tasks_row, table, hidden, pre_gain, frequency, post_gain,
    normed, queries, q_buf, k_buf, v_buf, w_buf, pool_buf, prompt_buf,
    onehot, onehot_t, valid, owned, page_query, qwide, page_mix, both, req_mix, packed, landed,
    fresh, fresh_rows, attended, sent, arrived, square, squares,
    small_sem, q_sem, k_sem, v_sem, w_sem, pool_sem, prompt_sem,
    query_send, query_recv, mix_send, mix_recv, part_send, part_recv, square_send, square_recv,
):
    me = lax.axis_index("seq")
    mine = lax.axis_index("tensor")
    rows, depth = hidden.shape
    cols = out.shape[1]
    requests = lengths.shape[1]
    q_width = q_buf.shape[1]
    kv_width = k_buf.shape[1]
    heads, kv_heads = q_width // hd, kv_width // hd
    group = heads // kv_heads
    pages, _, block_len, _ = pool.shape
    n_tasks, _, prompt_len, _ = prompts.shape
    max_blocks = table.shape[0]
    half = q_width // 2
    chunk = depth // steps

    smalls = []
    for i, (src, dst) in enumerate((
        (hidden_in, hidden), (pre_gain_in, pre_gain), (frequency_in, frequency),
        (lengths_in, lengths), (tasks_in, tasks), (tasks_row_in, tasks_row),
        (table_in, table), (post_gain_in, post_gain),
    )):
        smalls.append(pltpu.make_async_copy(src, dst, small_sem.at[i]))

    def q_copy(n, c):
        span, lanes = pl.ds(c * chunk, chunk), pl.ds(n * half, half)
        return pltpu.make_async_copy(
            w_query.at[span, lanes], q_buf.at[span, lanes], q_sem.at[n * steps + c]
        )

    def kv_copy(src, dst, sem, c):
        span = pl.ds(c * chunk, chunk)
        return pltpu.make_async_copy(src.at[span], dst.at[span], sem.at[c])

    def pool_copy(b):
        span = pl.ds(b * SLOTS, SLOTS)
        return pltpu.make_async_copy(pool.at[span], pool_buf.at[span], pool_sem.at[b])

    def prompt_copy(b):
        span = pl.ds(b * SLOTS, SLOTS)
        return pltpu.make_async_copy(prompts.at[span], prompt_buf.at[span], prompt_sem.at[b])

    def partners(i):
        return [3 - i, lax.rem(i + 2, 4), i + 1 - 2 * lax.rem(i, 2)]

    seq_peers = partners(me)
    tensor_peers = partners(mine)

    def w_copy(k):
        column = tensor_peers[k] if k < 3 else mine
        start = pl.multiple_of(column * cols, 128)
        return pltpu.make_async_copy(w_out.at[:, pl.ds(start, cols)], w_buf.at[k], w_sem.at[k])

    smalls[0].start()
    smalls[1].start()
    for n in range(2):
        for c in range(steps):
            q_copy(n, c).start()
        if n == 0:
            for copy in smalls[2:]:
                copy.start()
    for b in range(pages // SLOTS):
        pool_copy(b).start()
    for b in range(n_tasks // SLOTS):
        prompt_copy(b).start()
    for c in range(steps):
        kv_copy(w_key, k_buf, k_sem, c).start()
        kv_copy(w_value, v_buf, v_sem, c).start()
    for k in range(4):
        w_copy(k).start()

    barrier = pltpu.get_barrier_semaphore()
    for peer in seq_peers:
        pl.semaphore_signal(barrier, inc=1, device_id={"seq": peer}, device_id_type=MESH)
    for peer in tensor_peers:
        pl.semaphore_signal(barrier, inc=1, device_id={"tensor": peer}, device_id_type=MESH)

    qwide[...] = jnp.zeros_like(qwide)
    for copy in smalls:
        copy.wait()
    x = hidden[...].astype(jnp.float32)
    mean_square = jnp.mean(x * x, axis=-1, keepdims=True)
    normed[...] = (x * lax.rsqrt(mean_square + 1e-06) * pre_gain[...][None]).astype(jnp.bfloat16)

    row = lax.broadcasted_iota(jnp.int32, (rows, requests), 0)
    column = lax.broadcasted_iota(jnp.int32, (rows, requests), 1)
    own_length = jnp.sum(
        jnp.where(column == me * rows + row, lengths[...].astype(jnp.float32), 0.0),
        axis=1, keepdims=True,
    )
    angles = (own_length + prompt_len) * frequency[...]
    lane = lax.broadcasted_iota(jnp.int32, (rows, hd), 1)
    cos_all = jnp.cos(angles)
    sin_all = jnp.sin(angles)
    sin_all = jnp.where(lane < hd // 2, -sin_all, sin_all)

    query_copies = []
    for n in range(2):
        lanes = slice(n * half, (n + 1) * half)
        acc = None
        for c in range(steps):
            q_copy(n, c).wait()
            term = jnp.dot(
                normed[:, c * chunk : (c + 1) * chunk],
                q_buf[c * chunk : (c + 1) * chunk, lanes],
                preferred_element_type=jnp.float32,
            )
            acc = term if acc is None else acc + term
        turned = jnp.concatenate(
            [
                rope_lanes(acc[:, i * hd : (i + 1) * hd], cos_all, sin_all)
                for i in range(half // hd)
            ],
            axis=1,
        ).astype(jnp.bfloat16)
        queries[pl.ds(me, 1), :, lanes] = turned[None]
        if n == 0:
            pl.semaphore_wait(barrier, 6)
        for k, peer in enumerate(seq_peers):
            where = queries.at[me, :, pl.ds(n * half, half)]
            copy = pltpu.make_async_remote_copy(
                src_ref=where, dst_ref=where,
                send_sem=query_send.at[n * 3 + k], recv_sem=query_recv.at[n * 3 + k],
                device_id={"seq": peer}, device_id_type=MESH,
            )
            copy.start()
            query_copies.append(copy)

    page_id = me * pages + lax.broadcasted_iota(jnp.int32, (pages, requests), 0)

    def match_one(j, carry):
        hot, count = carry
        hit = jnp.broadcast_to(table[pl.ds(j, 1), :], (pages, requests)) == page_id
        tokens = jnp.broadcast_to(
            jnp.clip(lengths[...] - j * block_len, 0, block_len), (pages, requests)
        )
        return jnp.where(hit, 1.0, hot), jnp.where(hit, tokens.astype(jnp.float32), count)

    zeros = jnp.zeros((pages, requests), jnp.float32)
    hot, count = lax.fori_loop(0, max_blocks, match_one, (zeros, zeros))
    onehot[...] = hot.astype(jnp.bfloat16)
    turned = hot.T.astype(jnp.bfloat16)
    onehot_t[...] = jnp.concatenate([turned, turned], axis=1)
    valid[...] = jnp.broadcast_to(jnp.sum(count, axis=1, keepdims=True), valid.shape)
    line = lax.broadcasted_iota(jnp.int32, (requests, requests), 0)
    across = lax.broadcasted_iota(jnp.int32, (requests, requests), 1)
    local = tasks_row[...] - me * n_tasks
    is_owned = jnp.where((local >= 0) & (local < n_tasks), 1.0, 0.0)
    owned[...] = jnp.broadcast_to(
        jnp.sum(jnp.where(line == across, is_owned, 0.0), axis=1, keepdims=True), owned.shape
    )

    for copy in query_copies:
        copy.wait()
    all_queries = queries[...].reshape(requests, q_width)
    page_query[...] = jnp.dot(
        onehot[...], all_queries, preferred_element_type=jnp.float32
    ).astype(jnp.bfloat16)

    def widen(slot, source):
        for h in range(heads):
            kv = h // group
            qwide[slot, h * SLOTS : (h + 1) * SLOTS, kv * hd : (kv + 1) * hd] = source(
                slice(h * hd, (h + 1) * hd)
            )

    token = lax.broadcasted_iota(jnp.int32, (SLOTS, TOKENS), 1)

    def pool_step(step, carry):
        groups = []
        starts = []
        for s in range(2):
            g = step * 2 + s
            pool_copy(g).wait()
            start = pl.multiple_of(g * SLOTS, SLOTS)
            widen(s, lambda lanes, start=start: page_query[pl.ds(start, SLOTS), lanes])

            def load(which, start=start):
                def one(pair, t):
                    return pool_buf[
                        pl.ds(start + 2 * pair, 2), which, :, t * 256 : (t + 1) * 256
                    ].reshape(2 * block_len, 256)

                return one

            live = jnp.where(
                token.astype(jnp.float32) < valid[pl.ds(start, SLOTS), :], 1.0, 0.0
            )
            groups.append((qwide.at[s], load(0), load(1), SLOTS // 2, 1, live))
            starts.append(start)
        for start, result in zip(
            starts, attend_groups(groups, heads, kv_heads, hd, score_scale)
        ):
            for i, piece in enumerate(result):
                page_mix[pl.ds(start, SLOTS), i * hd : (i + 1) * hd] = piece
        return carry

    lax.fori_loop(0, pages // (2 * SLOTS), pool_step, 0)
    high = page_mix[...].astype(jnp.bfloat16)
    both[:pages, :] = high
    both[pages:, :] = (page_mix[...] - high.astype(jnp.float32)).astype(jnp.bfloat16)
    req_mix[...] = jnp.dot(onehot_t[...], both[...], preferred_element_type=jnp.float32)

    for b in range(n_tasks // SLOTS):
        prompt_copy(b).wait()
    per = TOKENS // prompt_len
    slot_of = lax.broadcasted_iota(jnp.int32, (SLOTS, TOKENS), 0)
    fits = token // prompt_len == slot_of % per
    mix_copies = []
    for k, peer in enumerate(seq_peers + [me]):
        groups = []
        for s in range(rows // SLOTS):
            first = peer * rows + s * SLOTS
            widen(s, lambda lanes, s=s: queries[peer, s * SLOTS : (s + 1) * SLOTS, lanes])
            places = [
                jnp.clip(tasks[first + i] - me * n_tasks, 0, n_tasks - 1) for i in range(SLOTS)
            ]

            def load(which, places=places):
                def one(pair, t):
                    return jnp.concatenate(
                        [
                            prompt_buf[place, which, :, t * 256 : (t + 1) * 256]
                            for place in places[pair * 2 * per : (pair + 1) * 2 * per]
                        ],
                        axis=0,
                    )

                return one

            start = pl.multiple_of(first, SLOTS)
            live = jnp.where(fits, owned[pl.ds(start, SLOTS), :], 0.0)
            groups.append((qwide.at[s], load(0), load(1), SLOTS // (2 * per), per, live))
        for s, result in enumerate(attend_groups(groups, heads, kv_heads, hd, score_scale)):
            start = pl.multiple_of(peer * rows + s * SLOTS, SLOTS)
            for i, piece in enumerate(result):
                lanes = slice(i * hd, (i + 1) * hd)
                sums = req_mix[pl.ds(start, SLOTS), lanes] + piece
                if k < 3:
                    packed[k, s * SLOTS : (s + 1) * SLOTS, lanes] = sums.astype(jnp.bfloat16)
                else:
                    req_mix[pl.ds(start, SLOTS), lanes] = sums
        if k < 3:
            copy = pltpu.make_async_remote_copy(
                src_ref=packed.at[k], dst_ref=landed.at[k],
                send_sem=mix_send.at[k], recv_sem=mix_recv.at[k],
                device_id={"seq": peer}, device_id_type=MESH,
            )
            copy.start()
            mix_copies.append(copy)

    kv_new = []
    for src, dst, sem in ((w_key, k_buf, k_sem), (w_value, v_buf, v_sem)):
        acc = None
        for c in range(steps):
            kv_copy(src, dst, sem, c).wait()
            term = jnp.dot(
                normed[:, c * chunk : (c + 1) * chunk],
                dst[c * chunk : (c + 1) * chunk, :],
                preferred_element_type=jnp.float32,
            )
            acc = term if acc is None else acc + term
        kv_new.append(acc)
    for g in range(kv_heads):
        lanes = slice(g * hd, (g + 1) * hd)
        fresh[0, :, lanes] = rope_lanes(kv_new[0][:, lanes], cos_all, sin_all).astype(jnp.bfloat16)
    fresh[1] = kv_new[1].astype(jnp.bfloat16)
    for i in range(2):
        fresh_rows[:, i, :] = fresh[i].astype(jnp.float32)
    fresh_out[...] = fresh_rows[...].astype(jnp.bfloat16)
    self_weights = []
    for h in range(heads):
        g = h // group
        q = queries[me, :, h * hd : (h + 1) * hd].astype(jnp.float32)
        k = fresh[0, :, g * hd : (g + 1) * hd].astype(jnp.float32)
        raw = jnp.sum(q * k, axis=1, keepdims=True)
        self_weights.append(jnp.exp(cap_limit * jnp.tanh(raw * (score_scale / cap_limit))))
    for copy in mix_copies:
        copy.wait()
    own = pl.ds(pl.multiple_of(me * rows, SLOTS), rows)
    totals = req_mix[own, q_width:]
    for k in range(3):
        totals += landed[k, :, q_width:].astype(jnp.float32)
    for h in range(heads):
        g = h // group
        lanes = slice(h * hd, (h + 1) * hd)
        mix = req_mix[own, lanes]
        for k in range(3):
            mix += landed[k, :, lanes].astype(jnp.float32)
        total = totals[:, h : h + 1] + self_weights[h]
        rounded = self_weights[h].astype(jnp.bfloat16).astype(jnp.float32)
        mix += rounded * fresh[1, :, g * hd : (g + 1) * hd].astype(jnp.float32)
        attended[:, lanes] = (mix / total).astype(jnp.bfloat16)

    parts = []
    for k in range(4):
        w_copy(k).wait()
        projected = jnp.dot(attended[...], w_buf[k], preferred_element_type=jnp.float32)
        if k < 3:
            sent[k] = projected.astype(jnp.bfloat16)
            copy = pltpu.make_async_remote_copy(
                src_ref=sent.at[k], dst_ref=arrived.at[k],
                send_sem=part_send.at[k], recv_sem=part_recv.at[k],
                device_id={"tensor": tensor_peers[k]}, device_id_type=MESH,
            )
            copy.start()
            parts.append(copy)
    whole = projected
    for k in (2, 0, 1):
        parts[k].wait()
        whole += arrived[k].astype(jnp.float32)
    part_square = jnp.sum(whole * whole, axis=1, keepdims=True)
    row = lax.broadcasted_iota(jnp.int32, (rows, 128), 0)
    diagonal = row == lax.broadcasted_iota(jnp.int32, (rows, 128), 1)
    square[...] = jnp.sum(jnp.where(diagonal, part_square, 0.0), axis=0, keepdims=True)
    copies = []
    for k, peer in enumerate(tensor_peers):
        copy = pltpu.make_async_remote_copy(
            src_ref=square, dst_ref=squares.at[k],
            send_sem=square_send.at[k], recv_sem=square_recv.at[k],
            device_id={"tensor": peer}, device_id_type=MESH,
        )
        copy.start()
        copies.append(copy)
    scaled = whole * post_gain[...][None]
    start = pl.multiple_of(mine * cols, 128)
    residual = hidden[:, pl.ds(start, cols)].astype(jnp.float32)
    for copy in copies:
        copy.wait()
    total_square = square[...]
    for k in range(3):
        total_square += squares[k]
    column_square = jnp.sum(jnp.where(diagonal, total_square, 0.0), axis=1, keepdims=True)
    factor = lax.rsqrt(column_square / (cols * tensor) + 1e-06)
    out[...] = (residual + scaled * factor).astype(jnp.bfloat16)


STEPS = 3


def body(
    seq, tensor, hidden, pre_gain, w_query, w_key, w_value, w_out, post_gain,
    cache_pool, prompt_cache, task_ids, cache_lengths, block_table,
):
    rows, depth = hidden.shape
    requests = task_ids.shape[0]
    pages, _, _, kv_width = cache_pool.shape
    n_tasks = prompt_cache.shape[0]
    q_width = w_query.shape[1]
    heads = q_width // HD
    cols = post_gain.shape[0]
    score_scale = float(D // H) ** (-0.5)
    half = HD // 2
    frequency = 10000.0 ** (-np.arange(half) / half)
    frequency = jnp.asarray(np.concatenate([frequency, frequency])[None], jnp.float32)
    vmem = pl.BlockSpec(memory_space=pltpu.VMEM)
    hbm = pl.BlockSpec(memory_space=pl.ANY)
    dma = pltpu.SemaphoreType.DMA
    bf16, f32, i32 = jnp.bfloat16, jnp.float32, jnp.int32
    packed_width = q_width + HD
    return pl.pallas_call(
        functools.partial(layer_kernel, seq, tensor, score_scale, HD, STEPS),
        out_shape=(
            jax.ShapeDtypeStruct((rows, cols), bf16),
            jax.ShapeDtypeStruct((rows, 2, kv_width), bf16),
        ),
        in_specs=[hbm] * 14,
        out_specs=(vmem, vmem),
        scratch_shapes=[
            pltpu.VMEM((1, requests), i32),
            pltpu.SMEM((requests,), i32),
            pltpu.VMEM((1, requests), i32),
            pltpu.VMEM((block_table.shape[1], requests), i32),
            pltpu.VMEM((rows, depth), bf16),
            pltpu.VMEM((depth,), f32),
            pltpu.VMEM((1, HD), f32),
            pltpu.VMEM((cols,), f32),
            pltpu.VMEM((rows, depth), bf16),
            pltpu.VMEM((seq, rows, q_width), bf16),
            pltpu.VMEM((depth, q_width), bf16),
            pltpu.VMEM((depth, kv_width), bf16),
            pltpu.VMEM((depth, kv_width), bf16),
            pltpu.VMEM((tensor, w_out.shape[0], cols), bf16),
            pltpu.VMEM(cache_pool.shape, bf16),
            pltpu.VMEM(prompt_cache.shape, bf16),
            pltpu.VMEM((pages, requests), bf16),
            pltpu.VMEM((requests, 2 * pages), bf16),
            pltpu.VMEM((pages, TOKENS), f32),
            pltpu.VMEM((requests, TOKENS), f32),
            pltpu.VMEM((pages, q_width), bf16),
            pltpu.VMEM((2, heads * SLOTS, kv_width), bf16),
            pltpu.VMEM((pages, packed_width), f32),
            pltpu.VMEM((2 * pages, packed_width), bf16),
            pltpu.VMEM((requests, packed_width), f32),
            pltpu.VMEM((3, rows, packed_width), bf16),
            pltpu.VMEM((3, rows, packed_width), bf16),
            pltpu.VMEM((2, rows, kv_width), bf16),
            pltpu.VMEM((rows, 2, kv_width), f32),
            pltpu.VMEM((rows, q_width), bf16),
            pltpu.VMEM((3, rows, cols), bf16),
            pltpu.VMEM((3, rows, cols), bf16),
            pltpu.VMEM((1, 128), f32),
            pltpu.VMEM((3, 1, 128), f32),
            dma((8,)),
            dma((2 * STEPS,)),
            dma((STEPS,)),
            dma((STEPS,)),
            dma((tensor,)),
            dma((pages // SLOTS,)),
            dma((n_tasks // SLOTS,)),
            dma((6,)),
            dma((6,)),
            dma((3,)),
            dma((3,)),
            dma((3,)),
            dma((3,)),
            dma((3,)),
            dma((3,)),
        ],
        compiler_params=pltpu.CompilerParams(
            collective_id=0, has_side_effects=True, vmem_limit_bytes=VMEM_BYTES
        ),
    )(
        cache_lengths.reshape(1, -1), task_ids, task_ids.reshape(1, -1), block_table.T,
        hidden, pre_gain, frequency, post_gain,
        w_query, w_key, w_value, w_out, cache_pool, prompt_cache,
    )


def fits(seq, tensor, arrays):
    hidden, w_query, w_key, post_gain = arrays[0], arrays[2], arrays[3], arrays[6]
    pool, prompts, tasks = arrays[7], arrays[8], arrays[9]
    return (
        seq == 4
        and tensor == 4
        and hidden.shape[0] == 2 * SLOTS
        and hidden.shape[1] % (STEPS * 256) == 0
        and w_query.shape[1] % 256 == 0
        and w_key.shape[1] % 256 == 0
        and w_query.shape[1] % w_key.shape[1] == 0
        and post_gain.shape[0] % 128 == 0
        and pool.shape[0] == 64
        and pool.shape[2] == TOKENS
        and prompts.shape[0] % SLOTS == 0
        and prompts.shape[2] == TOKENS // 2
        and tasks.shape[0] == 128
    )


def solution(mesh):
    seq, tensor = mesh.shape["seq"], mesh.shape["tensor"]

    def chosen(*arrays):
        if not fits(seq, tensor, arrays):
            return plain_body(*arrays)
        return body(seq, tensor, *arrays)

    return jax.shard_map(
        chosen,
        mesh=mesh,
        in_specs=(
            P(("groups", "seq"), None),
            P(),
            P(None, "tensor"),
            P(None, "tensor"),
            P(None, "tensor"),
            P("tensor", None),
            P("tensor"),
            P(("groups", "seq"), None, None, "tensor"),
            P("seq", None, None, "tensor"),
            P("groups"),
            P("groups"),
            P("groups", None),
        ),
        out_specs=(P(("groups", "seq"), "tensor"), P(("groups", "seq"), None, "tensor")),
        check_vma=False,
    )
```

```python
import jax
import jax.numpy as jnp
from jax import lax
from jax.experimental import pallas as pl
from jax.experimental.pallas import tpu as pltpu
from jax.sharding import PartitionSpec as P
import functools
import numpy as np

D = 4608
H = 32
HD = 128


cap_limit = 50.0


def rms_scale(values, gain):
    mean_square = jnp.mean(values * values, axis=-1, keepdims=True)
    return values * lax.rsqrt(mean_square + 1e-06) * gain


def rotate(values, position):
    half_dim = values.shape[-1] // 2
    frequency = 10000.0 ** (-jnp.arange(half_dim, dtype=jnp.float32) / half_dim)
    angles = position.astype(jnp.float32)[:, None] * frequency[None, :]
    cosine = jnp.cos(angles)[:, None, :]
    sines = jnp.sin(angles)[:, None, :]
    first_half = values[..., :half_dim]
    second_half = values[..., half_dim:]
    return jnp.concatenate(
        [first_half * cosine - second_half * sines, second_half * cosine + first_half * sines],
        axis=-1,
    )


def capped(raw_score, score_scale):
    return cap_limit * jnp.tanh(raw_score * score_scale / cap_limit)


def attend(query_block, block, live_mask, score_scale):
    count = block.shape[0]
    length = block.shape[2]
    kv_heads = query_block.shape[1]
    head_dim = query_block.shape[3]
    block_keys = block[:, 0].reshape(count, length, kv_heads, head_dim)
    block_values = block[:, 1].reshape(count, length, kv_heads, head_dim)
    raw_score = jnp.einsum(
        "nkgd,ntkd->nkgt", query_block, block_keys, preferred_element_type=jnp.float32
    )
    weight = jnp.where(live_mask[:, None, None, :], jnp.exp(capped(raw_score, score_scale)), 0.0)
    totals = jnp.sum(weight, axis=-1).reshape(count, -1)
    mixtures = jnp.einsum(
        "nkgt,ntkd->nkgd",
        weight.astype(jnp.bfloat16),
        block_values,
        preferred_element_type=jnp.float32,
    )
    return (totals, mixtures.reshape(count, -1))


def plain_body(
    hidden,
    pre_gain,
    w_query,
    w_key,
    w_value,
    w_out,
    post_gain,
    cache_pool,
    prompt_cache,
    task_ids,
    cache_lengths,
    block_table,
):
    seq_index = lax.axis_index("seq")
    tensor_index = lax.axis_index("tensor")
    own_rows = hidden.shape[0]
    requests = task_ids.shape[0]
    pages_dev = cache_pool.shape[0]
    block_len = cache_pool.shape[2]
    kv_width = cache_pool.shape[3]
    head_dim = HD
    kv_heads = kv_width // head_dim
    query_heads = w_query.shape[1] // head_dim
    group_size = query_heads // kv_heads
    prompt_len = prompt_cache.shape[2]
    tasks_dev = prompt_cache.shape[0]
    score_scale = float(D // H) ** (-0.5)
    first_row = seq_index * own_rows
    own_lengths = lax.dynamic_slice_in_dim(cache_lengths, first_row, own_rows)
    normed = rms_scale(hidden.astype(jnp.float32), pre_gain).astype(jnp.bfloat16)
    position = prompt_len + own_lengths
    query_rows = rotate(
        jnp.dot(normed, w_query, preferred_element_type=jnp.float32).reshape(
            own_rows, query_heads, head_dim
        ),
        position,
    ).astype(jnp.bfloat16)
    key_new = rotate(
        jnp.dot(normed, w_key, preferred_element_type=jnp.float32).reshape(
            own_rows, kv_heads, head_dim
        ),
        position,
    ).astype(jnp.bfloat16)
    value_new = jnp.dot(normed, w_value, preferred_element_type=jnp.float32).astype(jnp.bfloat16)
    fresh_cache = jnp.stack([key_new.reshape(own_rows, kv_width), value_new], axis=1)
    queries = lax.all_gather(
        query_rows.reshape(own_rows, query_heads * head_dim), "seq", axis=0, tiled=True
    )
    page_ids = seq_index * pages_dev + jnp.arange(pages_dev)
    flat_table = block_table.reshape(-1)
    max_blocks = block_table.shape[1]
    matches = flat_table[None, :] == page_ids[:, None]
    entry_index = jnp.arange(flat_table.shape[0])
    page_used = jnp.any(matches, axis=1)
    found_entry = jnp.sum(jnp.where(matches, entry_index[None, :], 0), axis=1)
    page_owner = found_entry // max_blocks
    block_number = found_entry % max_blocks
    owner_hot = (page_owner[:, None] == jnp.arange(requests)[None, :]) & page_used[:, None]
    owner_length = jnp.sum(jnp.where(owner_hot, cache_lengths[None, :], 0), axis=1)
    valid_count = jnp.clip(owner_length - block_number * block_len, 0, block_len)
    page_query = jnp.dot(
        owner_hot.astype(jnp.bfloat16), queries, preferred_element_type=jnp.float32
    ).astype(jnp.bfloat16)
    page_query = page_query.reshape(pages_dev, kv_heads, group_size, head_dim)
    page_live = jnp.arange(block_len)[None, :] < valid_count[:, None]
    page_totals, page_mixtures = attend(page_query, cache_pool, page_live, score_scale)
    spread_hot = owner_hot.astype(jnp.float32).T
    totals = jnp.dot(spread_hot, page_totals, precision=lax.Precision.HIGHEST)
    mixtures = jnp.dot(spread_hot, page_mixtures, precision=lax.Precision.HIGHEST)
    local_task = task_ids - seq_index * tasks_dev
    is_owned = (local_task >= 0) & (local_task < tasks_dev)
    task_rows = prompt_cache[jnp.clip(local_task, 0, tasks_dev - 1)]
    all_query = queries.reshape(requests, kv_heads, group_size, head_dim)
    owned_live = jnp.broadcast_to(is_owned[:, None], (requests, prompt_len))
    prompt_totals, prompt_mixtures = attend(all_query, task_rows, owned_live, score_scale)
    totals = totals + prompt_totals
    mixtures = mixtures + prompt_mixtures
    totals, mixtures = (
        lax.psum_scatter(
            totals.astype(jnp.bfloat16), "seq", scatter_dimension=0, tiled=True
        ).astype(jnp.float32),
        lax.psum_scatter(
            mixtures.astype(jnp.bfloat16), "seq", scatter_dimension=0, tiled=True
        ).astype(jnp.float32),
    )
    own_query = query_rows.reshape(own_rows, kv_heads, group_size, head_dim)
    self_raw = jnp.sum(
        own_query.astype(jnp.float32) * key_new[:, :, None, :].astype(jnp.float32), axis=-1
    )
    self_weight = jnp.exp(capped(self_raw, score_scale))
    rounded = lax.optimization_barrier(self_weight.astype(jnp.bfloat16)).astype(jnp.float32)
    totals = totals + self_weight.reshape(own_rows, -1)
    self_mix = rounded[..., None] * value_new.reshape(own_rows, kv_heads, 1, head_dim).astype(
        jnp.float32
    )
    mixtures = mixtures + self_mix.reshape(own_rows, -1)
    attended = (mixtures.reshape(own_rows, query_heads, head_dim) / totals[..., None]).astype(
        jnp.bfloat16
    )
    projected = jnp.dot(
        attended.reshape(own_rows, query_heads * head_dim),
        w_out,
        preferred_element_type=jnp.float32,
    )
    cols_local = post_gain.shape[0]
    col_start = tensor_index * cols_local
    residual = lax.dynamic_slice_in_dim(hidden, col_start, cols_local, 1).astype(jnp.float32)
    whole_sum = lax.psum(projected.astype(jnp.bfloat16), "tensor").astype(jnp.float32)
    mean_square = jnp.mean(whole_sum * whole_sum, axis=1, keepdims=True)
    scaled = lax.dynamic_slice_in_dim(whole_sum, col_start, cols_local, 1) * lax.rsqrt(
        mean_square + 1e-06
    )
    layer_out = (residual + scaled * post_gain).astype(jnp.bfloat16)
    return (layer_out, fresh_cache)


MESH = pl.DeviceIdType.MESH
VMEM_BYTES = 62 * 1024 * 1024


def rope_lanes(x, cosine, sines):
    return x * cosine + pltpu.roll(x, x.shape[-1] // 2, 1) * sines


SLOTS = 16
TOKENS = 128


def stacked(x, count):
    return jnp.concatenate([x] * count, axis=0)


def slot_unit(per):
    return lax.broadcasted_iota(jnp.int32, (SLOTS, TOKENS), 0) // per


def group_scores(sizes, qwide, keys, values, pairs, per, live):
    heads, kv_heads, hd, score_scale = sizes
    tiles = kv_heads * hd // 256
    tile_heads = heads // tiles
    rows = tile_heads * SLOTS
    unit = stacked(slot_unit(per), tile_heads)
    across = lax.broadcasted_iota(jnp.int32, (TOKENS, tiles * rows), 1) % SLOTS // per
    held, streamed = [None] * tiles, None
    for pair in range(pairs):
        raws = []
        for t in range(tiles):
            q = qwide[t * rows : (t + 1) * rows, t * 256 : (t + 1) * 256]
            two = (keys(pair, t), q) if pair % 2 == 0 else (q, keys(pair, t))
            raws.append(
                lax.dot_general(
                    *two, (((1,), (1,)), ((), ())), preferred_element_type=jnp.float32
                )
            )
        if pair % 2 == 0:
            raw = jnp.concatenate(raws, axis=1)
            for u in range(2):
                part = raw[u * TOKENS : (u + 1) * TOKENS]
                streamed = part if streamed is None else jnp.where(
                    across == 2 * pair + u, part, streamed
                )
        else:
            for t in range(tiles):
                for u in range(2):
                    part = raws[t][:, u * TOKENS : (u + 1) * TOKENS]
                    held[t] = part if held[t] is None else jnp.where(
                        unit == 2 * pair + u, part, held[t]
                    )
    turned = streamed.T
    from_streamed = unit // 2 % 2 == 0
    return [
        jnp.where(from_streamed, turned[t * rows : (t + 1) * rows], held[t]) for t in range(tiles)
    ]


def group_mixes(sizes, chosen, qwide, keys, values, pairs, per, live):
    heads, kv_heads, hd, score_scale = sizes
    tiles = kv_heads * hd // 256
    tile_heads = heads // tiles
    wide_live = stacked(live, tile_heads)
    mixes, totals = [], []
    for t in range(tiles):
        weight = jnp.exp(cap_limit * jnp.tanh(chosen[t] * (score_scale / cap_limit)))
        weight = jnp.where(wide_live > 0, weight, 0.0)
        total = jnp.sum(weight, axis=1, keepdims=True)
        narrow = weight.astype(jnp.bfloat16)
        acc = None
        for pair in range(pairs):
            pieces = []
            for u in range(2):
                keep = (slot_unit(per) == 2 * pair + u).astype(jnp.float32).astype(jnp.bfloat16)
                pieces.append(narrow * stacked(keep, tile_heads))
            term = jnp.dot(
                jnp.concatenate(pieces, axis=1), values(pair, t), preferred_element_type=jnp.float32
            )
            acc = term if acc is None else acc + term
        for i in range(tile_heads):
            span = slice(i * SLOTS, (i + 1) * SLOTS)
            kv = i // (heads // kv_heads)
            mixes.append(acc[span, kv * hd : (kv + 1) * hd])
            totals.append(total[span])
    lane = lax.broadcasted_iota(jnp.int32, (SLOTS, hd), 1)
    packed_total = jnp.zeros((SLOTS, hd), jnp.float32)
    for h in range(heads):
        packed_total = jnp.where(lane == h, totals[h], packed_total)
    return mixes + [packed_total]


def layer_kernel(
    seq, tensor, score_scale, hd, steps,
    lengths_in, tasks_in, tasks_row_in, table_in, hidden_in, pre_gain_in, frequency_in, post_gain_in,
    w_query, w_key, w_value, w_out, pool, prompts,
    out, fresh_out,
    lengths, tasks, tasks_row, table, hidden, pre_gain, frequency, post_gain,
    normed, queries, q_buf, k_buf, v_buf, w_buf, pool_buf, prompt_buf,
    onehot, onehot_t, valid, owned, page_query, qwide, page_mix, both, req_mix, packed, landed,
    fresh, fresh_rows, attended, sent, arrived, square, squares,
    small_sem, q_sem, k_sem, v_sem, w_sem, pool_sem, prompt_sem,
    query_send, query_recv, mix_send, mix_recv, part_send, part_recv, square_send, square_recv,
):
    me = lax.axis_index("seq")
    mine = lax.axis_index("tensor")
    rows, depth = hidden.shape
    cols = out.shape[1]
    requests = lengths.shape[1]
    q_width = q_buf.shape[1]
    kv_width = k_buf.shape[1]
    heads, kv_heads = q_width // hd, kv_width // hd
    group = heads // kv_heads
    pages, _, block_len, _ = pool.shape
    n_tasks, _, prompt_len, _ = prompts.shape
    max_blocks = table.shape[0]
    half = q_width // 2
    chunk = depth // steps

    smalls = []
    for i, (src, dst) in enumerate((
        (hidden_in, hidden), (pre_gain_in, pre_gain), (frequency_in, frequency),
        (lengths_in, lengths), (tasks_in, tasks), (tasks_row_in, tasks_row),
        (table_in, table), (post_gain_in, post_gain),
    )):
        smalls.append(pltpu.make_async_copy(src, dst, small_sem.at[i]))

    def q_copy(n, c):
        span, lanes = pl.ds(c * chunk, chunk), pl.ds(n * half, half)
        return pltpu.make_async_copy(
            w_query.at[span, lanes], q_buf.at[span, lanes], q_sem.at[n * steps + c]
        )

    def kv_copy(src, dst, sem, c):
        span = pl.ds(c * chunk, chunk)
        return pltpu.make_async_copy(src.at[span], dst.at[span], sem.at[c])

    def pool_copy(b):
        span = pl.ds(b * SLOTS, SLOTS)
        return pltpu.make_async_copy(pool.at[span], pool_buf.at[span], pool_sem.at[b])

    def prompt_copy(b):
        span = pl.ds(b * SLOTS, SLOTS)
        return pltpu.make_async_copy(prompts.at[span], prompt_buf.at[span], prompt_sem.at[b])

    def partners(i):
        return [3 - i, lax.rem(i + 2, 4), i + 1 - 2 * lax.rem(i, 2)]

    seq_peers = partners(me)
    tensor_peers = partners(mine)

    w_rows = w_out.shape[0] // 2

    def w_copy(k, i):
        column = tensor_peers[k] if k < 3 else mine
        start = pl.multiple_of(column * cols, 128)
        span = pl.ds(i * w_rows, w_rows)
        return pltpu.make_async_copy(
            w_out.at[span, pl.ds(start, cols)], w_buf.at[k, span], w_sem.at[2 * k + i]
        )

    for copy in smalls:
        copy.start()

    def start_all(count, start_one):
        def one(i, carry):
            start_one(i)
            return carry

        lax.fori_loop(0, count, one, 0)

    for n in range(2):
        start_all(steps, lambda c, n=n: q_copy(n, c).start())
    start_all(pages // SLOTS, lambda b: pool_copy(b).start())
    start_all(n_tasks // SLOTS, lambda b: prompt_copy(b).start())
    start_all(steps, lambda c: kv_copy(w_key, k_buf, k_sem, c).start())
    start_all(steps, lambda c: kv_copy(w_value, v_buf, v_sem, c).start())
    for k in range(4):
        start_all(2, lambda i, k=k: w_copy(k, i).start())

    barrier = pltpu.get_barrier_semaphore()
    for peer in seq_peers:
        pl.semaphore_signal(barrier, inc=1, device_id={"seq": peer}, device_id_type=MESH)
    for peer in tensor_peers:
        pl.semaphore_signal(barrier, inc=1, device_id={"tensor": peer}, device_id_type=MESH)

    qwide[...] = jnp.zeros_like(qwide)
    for copy in smalls:
        copy.wait()
    x = hidden[...].astype(jnp.float32)
    mean_square = jnp.mean(x * x, axis=-1, keepdims=True)
    normed[...] = (x * lax.rsqrt(mean_square + 1e-06) * pre_gain[...][None]).astype(jnp.bfloat16)

    row = lax.broadcasted_iota(jnp.int32, (rows, requests), 0)
    column = lax.broadcasted_iota(jnp.int32, (rows, requests), 1)
    own_length = jnp.sum(
        jnp.where(column == me * rows + row, lengths[...].astype(jnp.float32), 0.0),
        axis=1, keepdims=True,
    )
    angles = (own_length + prompt_len) * frequency[...]
    lane = lax.broadcasted_iota(jnp.int32, (rows, hd), 1)
    cos_all = jnp.cos(angles)
    sin_all = jnp.sin(angles)
    sin_all = jnp.where(lane < hd // 2, -sin_all, sin_all)

    query_copies = []
    for n in range(2):
        lanes = slice(n * half, (n + 1) * half)
        acc = None
        for c in range(steps):
            q_copy(n, c).wait()
            term = jnp.dot(
                normed[:, c * chunk : (c + 1) * chunk],
                q_buf[c * chunk : (c + 1) * chunk, lanes],
                preferred_element_type=jnp.float32,
            )
            acc = term if acc is None else acc + term
        turned = jnp.concatenate(
            [
                rope_lanes(acc[:, i * hd : (i + 1) * hd], cos_all, sin_all)
                for i in range(half // hd)
            ],
            axis=1,
        ).astype(jnp.bfloat16)
        queries[pl.ds(me, 1), :, lanes] = turned[None]
        if n == 0:
            pl.semaphore_wait(barrier, 6)
        for k, peer in enumerate(seq_peers):
            where = queries.at[me, :, pl.ds(n * half, half)]
            copy = pltpu.make_async_remote_copy(
                src_ref=where, dst_ref=where,
                send_sem=query_send.at[n * 3 + k], recv_sem=query_recv.at[n * 3 + k],
                device_id={"seq": peer}, device_id_type=MESH,
            )
            copy.start()
            query_copies.append(copy)

    page_id = me * pages + lax.broadcasted_iota(jnp.int32, (pages, requests), 0)

    def match_one(j, carry):
        hot, count = carry
        hit = jnp.broadcast_to(table[pl.ds(j, 1), :], (pages, requests)) == page_id
        tokens = jnp.broadcast_to(
            jnp.clip(lengths[...] - j * block_len, 0, block_len), (pages, requests)
        )
        return jnp.where(hit, 1.0, hot), jnp.where(hit, tokens.astype(jnp.float32), count)

    zeros = jnp.zeros((pages, requests), jnp.float32)
    hot, count = lax.fori_loop(0, max_blocks, match_one, (zeros, zeros))
    onehot[...] = hot.astype(jnp.bfloat16)
    turned = hot.T.astype(jnp.bfloat16)
    onehot_t[...] = jnp.concatenate([turned, turned], axis=1)
    valid[...] = jnp.broadcast_to(jnp.sum(count, axis=1, keepdims=True), valid.shape)
    line = lax.broadcasted_iota(jnp.int32, (requests, requests), 0)
    across = lax.broadcasted_iota(jnp.int32, (requests, requests), 1)
    local = tasks_row[...] - me * n_tasks
    is_owned = jnp.where((local >= 0) & (local < n_tasks), 1.0, 0.0)
    owned[...] = jnp.broadcast_to(
        jnp.sum(jnp.where(line == across, is_owned, 0.0), axis=1, keepdims=True), owned.shape
    )

    for copy in query_copies:
        copy.wait()
    all_queries = queries[...].reshape(requests, q_width)
    page_query[...] = jnp.dot(
        onehot[...], all_queries, preferred_element_type=jnp.float32
    ).astype(jnp.bfloat16)

    def widen(slot, source):
        for h in range(heads):
            kv = h // group
            qwide[slot, h * SLOTS : (h + 1) * SLOTS, kv * hd : (kv + 1) * hd] = source(
                slice(h * hd, (h + 1) * hd)
            )

    token = lax.broadcasted_iota(jnp.int32, (SLOTS, TOKENS), 1)

    sizes = (heads, kv_heads, hd, score_scale)
    per = TOKENS // prompt_len
    slot_of = lax.broadcasted_iota(jnp.int32, (SLOTS, TOKENS), 0)
    fits = token // prompt_len == slot_of % per
    pool_groups = pages // SLOTS
    halves = rows // SLOTS
    takers = seq_peers + [me]

    def pool_group(g):
        start = g * SLOTS
        widen(g % 4, lambda lanes: page_query[start : start + SLOTS, lanes])

        def load(which):
            def one(pair, t):
                first = start + 2 * pair
                return pool_buf[first : first + 2, which, :, t * 256 : (t + 1) * 256].reshape(
                    2 * block_len, 256
                )

            return one

        live = jnp.where(token.astype(jnp.float32) < valid[start : start + SLOTS, :], 1.0, 0.0)
        return (qwide.at[g % 4], load(0), load(1), SLOTS // 2, 1, live)

    def prompt_group(k, s):
        peer = takers[k]
        first = peer * rows + s * SLOTS
        slot = (k % 2) * 2 + s
        widen(slot, lambda lanes: queries[peer, s * SLOTS : (s + 1) * SLOTS, lanes])
        places = [
            jnp.clip(tasks[first + i] - me * n_tasks, 0, n_tasks - 1) for i in range(SLOTS)
        ]

        def load(which):
            def one(pair, t):
                return jnp.concatenate(
                    [
                        prompt_buf[place, which, :, t * 256 : (t + 1) * 256]
                        for place in places[pair * 2 * per : (pair + 1) * 2 * per]
                    ],
                    axis=0,
                )

            return one

        start = pl.multiple_of(first, SLOTS)
        live = jnp.where(fits, owned[pl.ds(start, SLOTS), :], 0.0)
        return (qwide.at[slot], load(0), load(1), SLOTS // (2 * per), per, live)

    def scores_of(made):
        return [(group, group_scores(sizes, *group)) for group in made]

    def finish_pool(g, scored):
        (group, chosen), = scored
        for i, piece in enumerate(group_mixes(sizes, chosen, *group)):
            page_mix[g * SLOTS : (g + 1) * SLOTS, i * hd : (i + 1) * hd] = piece

    mix_copies = []

    def finish_prompt(k, scored):
        peer = takers[k]
        for s, (group, chosen) in enumerate(scored):
            start = pl.multiple_of(peer * rows + s * SLOTS, SLOTS)
            for i, piece in enumerate(group_mixes(sizes, chosen, *group)):
                lanes = slice(i * hd, (i + 1) * hd)
                sums = req_mix[pl.ds(start, SLOTS), lanes] + piece
                if k < 3:
                    packed[k, s * SLOTS : (s + 1) * SLOTS, lanes] = sums.astype(jnp.bfloat16)
                else:
                    req_mix[pl.ds(start, SLOTS), lanes] = sums
        if k < 3:
            copy = pltpu.make_async_remote_copy(
                src_ref=packed.at[k], dst_ref=landed.at[k],
                send_sem=mix_send.at[k], recv_sem=mix_recv.at[k],
                device_id={"seq": peer}, device_id_type=MESH,
            )
            copy.start()
            mix_copies.append(copy)

    scored = None
    for g in range(pool_groups):
        pool_copy(g).wait()
        later = scores_of([pool_group(g)])
        if g:
            finish_pool(g - 1, scored)
        scored = later
    for b in range(n_tasks // SLOTS):
        prompt_copy(b).wait()
    later = scores_of([prompt_group(0, s) for s in range(halves)])
    finish_pool(pool_groups - 1, scored)
    high = page_mix[...].astype(jnp.bfloat16)
    both[:pages, :] = high
    both[pages:, :] = (page_mix[...] - high.astype(jnp.float32)).astype(jnp.bfloat16)
    req_mix[...] = jnp.dot(onehot_t[...], both[...], preferred_element_type=jnp.float32)
    for k in range(1, len(takers)):
        scored = later
        later = scores_of([prompt_group(k, s) for s in range(halves)])
        finish_prompt(k - 1, scored)
    finish_prompt(len(takers) - 1, later)

    def kv_product(src, dst, sem):
        acc = None
        for c in range(steps):
            kv_copy(src, dst, sem, c).wait()
            term = jnp.dot(
                normed[:, c * chunk : (c + 1) * chunk],
                dst[c * chunk : (c + 1) * chunk, :],
                preferred_element_type=jnp.float32,
            )
            acc = term if acc is None else acc + term
        return acc

    key_new = kv_product(w_key, k_buf, k_sem)
    for g in range(kv_heads):
        lanes = slice(g * hd, (g + 1) * hd)
        fresh[0, :, lanes] = rope_lanes(key_new[:, lanes], cos_all, sin_all).astype(jnp.bfloat16)
    self_weights = []
    for h in range(heads):
        g = h // group
        q = queries[me, :, h * hd : (h + 1) * hd].astype(jnp.float32)
        k = fresh[0, :, g * hd : (g + 1) * hd].astype(jnp.float32)
        raw = jnp.sum(q * k, axis=1, keepdims=True)
        self_weights.append(jnp.exp(cap_limit * jnp.tanh(raw * (score_scale / cap_limit))))
    fresh[1] = kv_product(w_value, v_buf, v_sem).astype(jnp.bfloat16)
    for i in range(2):
        fresh_rows[:, i, :] = fresh[i].astype(jnp.float32)
    fresh_out[...] = fresh_rows[...].astype(jnp.bfloat16)
    for copy in mix_copies:
        copy.wait()
    own = pl.ds(pl.multiple_of(me * rows, SLOTS), rows)
    totals = req_mix[own, q_width:]
    for k in range(3):
        totals += landed[k, :, q_width:].astype(jnp.float32)
    for h in range(heads):
        g = h // group
        lanes = slice(h * hd, (h + 1) * hd)
        mix = req_mix[own, lanes]
        for k in range(3):
            mix += landed[k, :, lanes].astype(jnp.float32)
        total = totals[:, h : h + 1] + self_weights[h]
        rounded = self_weights[h].astype(jnp.bfloat16).astype(jnp.float32)
        mix += rounded * fresh[1, :, g * hd : (g + 1) * hd].astype(jnp.float32)
        attended[:, lanes] = (mix / total).astype(jnp.bfloat16)

    parts = []
    for k in range(4):
        for i in range(2):
            w_copy(k, i).wait()
        projected = jnp.dot(attended[...], w_buf[k], preferred_element_type=jnp.float32)
        if k < 3:
            sent[k] = projected.astype(jnp.bfloat16)
            copy = pltpu.make_async_remote_copy(
                src_ref=sent.at[k], dst_ref=arrived.at[k],
                send_sem=part_send.at[k], recv_sem=part_recv.at[k],
                device_id={"tensor": tensor_peers[k]}, device_id_type=MESH,
            )
            copy.start()
            parts.append(copy)
    whole = projected
    for k in (2, 0, 1):
        parts[k].wait()
        whole += arrived[k].astype(jnp.float32)
    part_square = jnp.sum(whole * whole, axis=1, keepdims=True)
    row = lax.broadcasted_iota(jnp.int32, (rows, 128), 0)
    diagonal = row == lax.broadcasted_iota(jnp.int32, (rows, 128), 1)
    square[...] = jnp.sum(jnp.where(diagonal, part_square, 0.0), axis=0, keepdims=True)
    copies = []
    for k, peer in enumerate(tensor_peers):
        copy = pltpu.make_async_remote_copy(
            src_ref=square, dst_ref=squares.at[k],
            send_sem=square_send.at[k], recv_sem=square_recv.at[k],
            device_id={"tensor": peer}, device_id_type=MESH,
        )
        copy.start()
        copies.append(copy)
    scaled = whole * post_gain[...][None]
    start = pl.multiple_of(mine * cols, 128)
    residual = hidden[:, pl.ds(start, cols)].astype(jnp.float32)
    for copy in copies:
        copy.wait()
    total_square = square[...]
    for k in range(3):
        total_square += squares[k]
    column_square = jnp.sum(jnp.where(diagonal, total_square, 0.0), axis=1, keepdims=True)
    factor = lax.rsqrt(column_square / (cols * tensor) + 1e-06)
    out[...] = (residual + scaled * factor).astype(jnp.bfloat16)


STEPS = 3


def place_kernel(layer_in, fresh_in, layer_out, fresh_out, sems):
    copies = [
        pltpu.make_async_copy(layer_in, layer_out, sems.at[0]),
        pltpu.make_async_copy(fresh_in, fresh_out, sems.at[1]),
    ]
    for copy in copies:
        copy.start()
    for copy in copies:
        copy.wait()


def body(
    seq, tensor, hidden, pre_gain, w_query, w_key, w_value, w_out, post_gain,
    cache_pool, prompt_cache, task_ids, cache_lengths, block_table,
):
    rows, depth = hidden.shape
    requests = task_ids.shape[0]
    pages, _, _, kv_width = cache_pool.shape
    n_tasks = prompt_cache.shape[0]
    q_width = w_query.shape[1]
    heads = q_width // HD
    cols = post_gain.shape[0]
    score_scale = float(D // H) ** (-0.5)
    half = HD // 2
    frequency = 10000.0 ** (-np.arange(half) / half)
    frequency = jnp.asarray(np.concatenate([frequency, frequency])[None], jnp.float32)
    vmem = pl.BlockSpec(memory_space=pltpu.VMEM)
    hbm = pl.BlockSpec(memory_space=pl.ANY)
    dma = pltpu.SemaphoreType.DMA
    bf16, f32, i32 = jnp.bfloat16, jnp.float32, jnp.int32
    packed_width = q_width + HD
    layer_out, fresh = pl.pallas_call(
        functools.partial(layer_kernel, seq, tensor, score_scale, HD, STEPS),
        out_shape=(
            pltpu.VMEM((rows, cols), bf16),
            pltpu.VMEM((rows, 2, kv_width), bf16),
        ),
        in_specs=[hbm] * 14,
        out_specs=(vmem, vmem),
        scratch_shapes=[
            pltpu.VMEM((1, requests), i32),
            pltpu.SMEM((requests,), i32),
            pltpu.VMEM((1, requests), i32),
            pltpu.VMEM((block_table.shape[1], requests), i32),
            pltpu.VMEM((rows, depth), bf16),
            pltpu.VMEM((depth,), f32),
            pltpu.VMEM((1, HD), f32),
            pltpu.VMEM((cols,), f32),
            pltpu.VMEM((rows, depth), bf16),
            pltpu.VMEM((seq, rows, q_width), bf16),
            pltpu.VMEM((depth, q_width), bf16),
            pltpu.VMEM((depth, kv_width), bf16),
            pltpu.VMEM((depth, kv_width), bf16),
            pltpu.VMEM((tensor, w_out.shape[0], cols), bf16),
            pltpu.VMEM(cache_pool.shape, bf16),
            pltpu.VMEM(prompt_cache.shape, bf16),
            pltpu.VMEM((pages, requests), bf16),
            pltpu.VMEM((requests, 2 * pages), bf16),
            pltpu.VMEM((pages, TOKENS), f32),
            pltpu.VMEM((requests, TOKENS), f32),
            pltpu.VMEM((pages, q_width), bf16),
            pltpu.VMEM((4, heads * SLOTS, kv_width), bf16),
            pltpu.VMEM((pages, packed_width), f32),
            pltpu.VMEM((2 * pages, packed_width), bf16),
            pltpu.VMEM((requests, packed_width), f32),
            pltpu.VMEM((3, rows, packed_width), bf16),
            pltpu.VMEM((3, rows, packed_width), bf16),
            pltpu.VMEM((2, rows, kv_width), bf16),
            pltpu.VMEM((rows, 2, kv_width), f32),
            pltpu.VMEM((rows, q_width), bf16),
            pltpu.VMEM((3, rows, cols), bf16),
            pltpu.VMEM((3, rows, cols), bf16),
            pltpu.VMEM((1, 128), f32),
            pltpu.VMEM((3, 1, 128), f32),
            dma((8,)),
            dma((2 * STEPS,)),
            dma((STEPS,)),
            dma((STEPS,)),
            dma((2 * tensor,)),
            dma((pages // SLOTS,)),
            dma((n_tasks // SLOTS,)),
            dma((6,)),
            dma((6,)),
            dma((3,)),
            dma((3,)),
            dma((3,)),
            dma((3,)),
            dma((3,)),
            dma((3,)),
        ],
        compiler_params=pltpu.CompilerParams(
            collective_id=0, has_side_effects=True, vmem_limit_bytes=VMEM_BYTES
        ),
    )(
        cache_lengths.reshape(1, -1), task_ids, task_ids.reshape(1, -1), block_table.T,
        hidden, pre_gain, frequency, post_gain,
        w_query, w_key, w_value, w_out, cache_pool, prompt_cache,
    )
    return pl.pallas_call(
        place_kernel,
        out_shape=(
            jax.ShapeDtypeStruct((rows, cols), bf16),
            jax.ShapeDtypeStruct((rows, 2, kv_width), bf16),
        ),
        in_specs=[vmem, vmem],
        out_specs=(hbm, hbm),
        scratch_shapes=[dma((2,))],
        compiler_params=pltpu.CompilerParams(vmem_limit_bytes=1024 * 1024),
    )(layer_out, fresh)


def fits(seq, tensor, arrays):
    hidden, w_query, w_key, post_gain = arrays[0], arrays[2], arrays[3], arrays[6]
    pool, prompts, tasks = arrays[7], arrays[8], arrays[9]
    return (
        seq == 4
        and tensor == 4
        and hidden.shape[0] == 2 * SLOTS
        and hidden.shape[1] % (STEPS * 256) == 0
        and w_query.shape[1] % 256 == 0
        and w_key.shape[1] % 256 == 0
        and w_query.shape[1] % w_key.shape[1] == 0
        and post_gain.shape[0] % 128 == 0
        and pool.shape[0] == 64
        and pool.shape[2] == TOKENS
        and prompts.shape[0] % SLOTS == 0
        and prompts.shape[2] == TOKENS // 2
        and tasks.shape[0] == 128
    )


def solution(mesh):
    seq, tensor = mesh.shape["seq"], mesh.shape["tensor"]

    def chosen(*arrays):
        if not fits(seq, tensor, arrays):
            return plain_body(*arrays)
        return body(seq, tensor, *arrays)

    return jax.shard_map(
        chosen,
        mesh=mesh,
        in_specs=(
            P(("groups", "seq"), None),
            P(),
            P(None, "tensor"),
            P(None, "tensor"),
            P(None, "tensor"),
            P("tensor", None),
            P("tensor"),
            P(("groups", "seq"), None, None, "tensor"),
            P("seq", None, None, "tensor"),
            P("groups"),
            P("groups"),
            P("groups", None),
        ),
        out_specs=(P(("groups", "seq"), "tensor"), P(("groups", "seq"), None, "tensor")),
        check_vma=False,
    )
```

```python
import jax
import jax.numpy as jnp
from jax import lax
from jax.experimental import pallas as pl
from jax.experimental.pallas import tpu as pltpu
from jax.sharding import PartitionSpec as P
import functools
import numpy as np

D = 4608
H = 32
HD = 128


cap_limit = 50.0


def rms_scale(values, gain):
    mean_square = jnp.mean(values * values, axis=-1, keepdims=True)
    return values * lax.rsqrt(mean_square + 1e-06) * gain


def rotate(values, position):
    half_dim = values.shape[-1] // 2
    frequency = 10000.0 ** (-jnp.arange(half_dim, dtype=jnp.float32) / half_dim)
    angles = position.astype(jnp.float32)[:, None] * frequency[None, :]
    cosine = jnp.cos(angles)[:, None, :]
    sines = jnp.sin(angles)[:, None, :]
    first_half = values[..., :half_dim]
    second_half = values[..., half_dim:]
    return jnp.concatenate(
        [first_half * cosine - second_half * sines, second_half * cosine + first_half * sines],
        axis=-1,
    )


def capped(raw_score, score_scale):
    return cap_limit * jnp.tanh(raw_score * score_scale / cap_limit)


def attend(query_block, block, live_mask, score_scale):
    count = block.shape[0]
    length = block.shape[2]
    kv_heads = query_block.shape[1]
    head_dim = query_block.shape[3]
    block_keys = block[:, 0].reshape(count, length, kv_heads, head_dim)
    block_values = block[:, 1].reshape(count, length, kv_heads, head_dim)
    raw_score = jnp.einsum(
        "nkgd,ntkd->nkgt", query_block, block_keys, preferred_element_type=jnp.float32
    )
    weight = jnp.where(live_mask[:, None, None, :], jnp.exp(capped(raw_score, score_scale)), 0.0)
    totals = jnp.sum(weight, axis=-1).reshape(count, -1)
    mixtures = jnp.einsum(
        "nkgt,ntkd->nkgd",
        weight.astype(jnp.bfloat16),
        block_values,
        preferred_element_type=jnp.float32,
    )
    return (totals, mixtures.reshape(count, -1))


def plain_body(
    hidden,
    pre_gain,
    w_query,
    w_key,
    w_value,
    w_out,
    post_gain,
    cache_pool,
    prompt_cache,
    task_ids,
    cache_lengths,
    block_table,
):
    seq_index = lax.axis_index("seq")
    tensor_index = lax.axis_index("tensor")
    own_rows = hidden.shape[0]
    requests = task_ids.shape[0]
    pages_dev = cache_pool.shape[0]
    block_len = cache_pool.shape[2]
    kv_width = cache_pool.shape[3]
    head_dim = HD
    kv_heads = kv_width // head_dim
    query_heads = w_query.shape[1] // head_dim
    group_size = query_heads // kv_heads
    prompt_len = prompt_cache.shape[2]
    tasks_dev = prompt_cache.shape[0]
    score_scale = float(D // H) ** (-0.5)
    first_row = seq_index * own_rows
    own_lengths = lax.dynamic_slice_in_dim(cache_lengths, first_row, own_rows)
    normed = rms_scale(hidden.astype(jnp.float32), pre_gain).astype(jnp.bfloat16)
    position = prompt_len + own_lengths
    query_rows = rotate(
        jnp.dot(normed, w_query, preferred_element_type=jnp.float32).reshape(
            own_rows, query_heads, head_dim
        ),
        position,
    ).astype(jnp.bfloat16)
    key_new = rotate(
        jnp.dot(normed, w_key, preferred_element_type=jnp.float32).reshape(
            own_rows, kv_heads, head_dim
        ),
        position,
    ).astype(jnp.bfloat16)
    value_new = jnp.dot(normed, w_value, preferred_element_type=jnp.float32).astype(jnp.bfloat16)
    fresh_cache = jnp.stack([key_new.reshape(own_rows, kv_width), value_new], axis=1)
    queries = lax.all_gather(
        query_rows.reshape(own_rows, query_heads * head_dim), "seq", axis=0, tiled=True
    )
    page_ids = seq_index * pages_dev + jnp.arange(pages_dev)
    flat_table = block_table.reshape(-1)
    max_blocks = block_table.shape[1]
    matches = flat_table[None, :] == page_ids[:, None]
    entry_index = jnp.arange(flat_table.shape[0])
    page_used = jnp.any(matches, axis=1)
    found_entry = jnp.sum(jnp.where(matches, entry_index[None, :], 0), axis=1)
    page_owner = found_entry // max_blocks
    block_number = found_entry % max_blocks
    owner_hot = (page_owner[:, None] == jnp.arange(requests)[None, :]) & page_used[:, None]
    owner_length = jnp.sum(jnp.where(owner_hot, cache_lengths[None, :], 0), axis=1)
    valid_count = jnp.clip(owner_length - block_number * block_len, 0, block_len)
    page_query = jnp.dot(
        owner_hot.astype(jnp.bfloat16), queries, preferred_element_type=jnp.float32
    ).astype(jnp.bfloat16)
    page_query = page_query.reshape(pages_dev, kv_heads, group_size, head_dim)
    page_live = jnp.arange(block_len)[None, :] < valid_count[:, None]
    page_totals, page_mixtures = attend(page_query, cache_pool, page_live, score_scale)
    spread_hot = owner_hot.astype(jnp.float32).T
    totals = jnp.dot(spread_hot, page_totals, precision=lax.Precision.HIGHEST)
    mixtures = jnp.dot(spread_hot, page_mixtures, precision=lax.Precision.HIGHEST)
    local_task = task_ids - seq_index * tasks_dev
    is_owned = (local_task >= 0) & (local_task < tasks_dev)
    task_rows = prompt_cache[jnp.clip(local_task, 0, tasks_dev - 1)]
    all_query = queries.reshape(requests, kv_heads, group_size, head_dim)
    owned_live = jnp.broadcast_to(is_owned[:, None], (requests, prompt_len))
    prompt_totals, prompt_mixtures = attend(all_query, task_rows, owned_live, score_scale)
    totals = totals + prompt_totals
    mixtures = mixtures + prompt_mixtures
    totals, mixtures = (
        lax.psum_scatter(
            totals.astype(jnp.bfloat16), "seq", scatter_dimension=0, tiled=True
        ).astype(jnp.float32),
        lax.psum_scatter(
            mixtures.astype(jnp.bfloat16), "seq", scatter_dimension=0, tiled=True
        ).astype(jnp.float32),
    )
    own_query = query_rows.reshape(own_rows, kv_heads, group_size, head_dim)
    self_raw = jnp.sum(
        own_query.astype(jnp.float32) * key_new[:, :, None, :].astype(jnp.float32), axis=-1
    )
    self_weight = jnp.exp(capped(self_raw, score_scale))
    rounded = lax.optimization_barrier(self_weight.astype(jnp.bfloat16)).astype(jnp.float32)
    totals = totals + self_weight.reshape(own_rows, -1)
    self_mix = rounded[..., None] * value_new.reshape(own_rows, kv_heads, 1, head_dim).astype(
        jnp.float32
    )
    mixtures = mixtures + self_mix.reshape(own_rows, -1)
    attended = (mixtures.reshape(own_rows, query_heads, head_dim) / totals[..., None]).astype(
        jnp.bfloat16
    )
    projected = jnp.dot(
        attended.reshape(own_rows, query_heads * head_dim),
        w_out,
        preferred_element_type=jnp.float32,
    )
    cols_local = post_gain.shape[0]
    col_start = tensor_index * cols_local
    residual = lax.dynamic_slice_in_dim(hidden, col_start, cols_local, 1).astype(jnp.float32)
    whole_sum = lax.psum(projected.astype(jnp.bfloat16), "tensor").astype(jnp.float32)
    mean_square = jnp.mean(whole_sum * whole_sum, axis=1, keepdims=True)
    scaled = lax.dynamic_slice_in_dim(whole_sum, col_start, cols_local, 1) * lax.rsqrt(
        mean_square + 1e-06
    )
    layer_out = (residual + scaled * post_gain).astype(jnp.bfloat16)
    return (layer_out, fresh_cache)


MESH = pl.DeviceIdType.MESH
VMEM_BYTES = 62 * 1024 * 1024


def rope_lanes(x, cosine, sines):
    return x * cosine + pltpu.roll(x, x.shape[-1] // 2, 1) * sines


SLOTS = 16
TOKENS = 128


def stacked(x, count):
    return jnp.concatenate([x] * count, axis=0)


def slot_unit(per):
    return lax.broadcasted_iota(jnp.int32, (SLOTS, TOKENS), 0) // per


def tile_scores(sizes, t, qwide, keys, values, pairs, per, live):
    heads, kv_heads, hd, score_scale = sizes
    tile_heads = heads * 256 // (kv_heads * hd)
    rows = tile_heads * SLOTS
    unit = stacked(slot_unit(per), tile_heads)
    across = lax.broadcasted_iota(jnp.int32, (TOKENS, rows), 1) % SLOTS // per
    q = qwide[t * rows : (t + 1) * rows, t * 256 : (t + 1) * 256]
    held, streamed = None, None
    for pair in range(pairs):
        two = (keys(pair, t), q) if pair % 2 == 0 else (q, keys(pair, t))
        raw = lax.dot_general(
            *two, (((1,), (1,)), ((), ())), preferred_element_type=jnp.float32
        )
        for u in range(2):
            if pair % 2 == 0:
                part = raw[u * TOKENS : (u + 1) * TOKENS]
                streamed = part if streamed is None else jnp.where(
                    across == 2 * pair + u, part, streamed
                )
            else:
                part = raw[:, u * TOKENS : (u + 1) * TOKENS]
                held = part if held is None else jnp.where(unit == 2 * pair + u, part, held)
    return jnp.where(unit // 2 % 2 == 0, streamed.T, held)


def tile_mixes(sizes, chosen, t, qwide, keys, values, pairs, per, live):
    heads, kv_heads, hd, score_scale = sizes
    tile_heads = heads * 256 // (kv_heads * hd)
    weight = jnp.exp(cap_limit * jnp.tanh(chosen * (score_scale / cap_limit)))
    weight = jnp.where(stacked(live, tile_heads) > 0, weight, 0.0)
    total = jnp.sum(weight, axis=1, keepdims=True)
    narrow = weight.astype(jnp.bfloat16)
    acc = None
    for pair in range(pairs):
        pieces = []
        for u in range(2):
            keep = (slot_unit(per) == 2 * pair + u).astype(jnp.float32).astype(jnp.bfloat16)
            pieces.append(narrow * stacked(keep, tile_heads))
        term = jnp.dot(
            jnp.concatenate(pieces, axis=1), values(pair, t), preferred_element_type=jnp.float32
        )
        acc = term if acc is None else acc + term
    mixes, totals = [], []
    for i in range(tile_heads):
        span = slice(i * SLOTS, (i + 1) * SLOTS)
        kv = i // (heads // kv_heads)
        mixes.append(acc[span, kv * hd : (kv + 1) * hd])
        totals.append(total[span])
    return mixes, totals


def group_mixes(sizes, scores, group):
    heads, hd = sizes[0], sizes[2]
    mixes, totals = [], []
    for t, chosen in enumerate(scores):
        more = tile_mixes(sizes, chosen, t, *group)
        mixes += more[0]
        totals += more[1]
    lane = lax.broadcasted_iota(jnp.int32, (SLOTS, hd), 1)
    packed_total = jnp.zeros((SLOTS, hd), jnp.float32)
    for h in range(heads):
        packed_total = jnp.where(lane == h, totals[h], packed_total)
    return mixes + [packed_total]


def layer_kernel(
    seq, tensor, score_scale, hd, steps,
    lengths_in, tasks_in, tasks_row_in, table_in, hidden_in, pre_gain_in, frequency_in, post_gain_in,
    w_query, w_key, w_value, w_out, pool, prompts,
    out, fresh_out,
    lengths, tasks, tasks_row, table, hidden, pre_gain, frequency, post_gain,
    normed, queries, q_buf, k_buf, v_buf, w_buf, pool_buf, prompt_buf,
    onehot, onehot_t, valid, owned, page_query, qwide, page_mix, both, req_mix, packed, landed,
    fresh, fresh_rows, attended, sent, arrived, held, whole_sum, square, squares,
    small_sem, q_sem, k_sem, v_sem, w_sem, pool_sem, prompt_sem,
    query_send, query_recv, mix_send, mix_recv, part_send, part_recv, square_send, square_recv,
):
    me = lax.axis_index("seq")
    mine = lax.axis_index("tensor")
    rows, depth = hidden.shape
    cols = out.shape[1]
    requests = lengths.shape[1]
    q_width = q_buf.shape[1]
    kv_width = k_buf.shape[1]
    heads, kv_heads = q_width // hd, kv_width // hd
    group = heads // kv_heads
    pages, _, block_len, _ = pool.shape
    n_tasks, _, prompt_len, _ = prompts.shape
    max_blocks = table.shape[0]
    half = q_width // 2
    chunk = depth // steps
    cut = cols // 256 * 128

    smalls = []
    for i, (src, dst) in enumerate((
        (hidden_in, hidden), (pre_gain_in, pre_gain), (frequency_in, frequency),
        (lengths_in, lengths), (tasks_in, tasks), (tasks_row_in, tasks_row),
        (table_in, table), (post_gain_in, post_gain),
    )):
        smalls.append(pltpu.make_async_copy(src, dst, small_sem.at[i]))

    def q_copy(n, c):
        span, lanes = pl.ds(c * chunk, chunk), pl.ds(n * half, half)
        return pltpu.make_async_copy(
            w_query.at[span, lanes], q_buf.at[span, lanes], q_sem.at[n * steps + c]
        )

    def kv_copy(src, dst, sem, c):
        span = pl.ds(c * chunk, chunk)
        return pltpu.make_async_copy(src.at[span], dst.at[span], sem.at[c])

    def pool_copy(b):
        span = pl.ds(b * SLOTS, SLOTS)
        return pltpu.make_async_copy(pool.at[span], pool_buf.at[span], pool_sem.at[b])

    def prompt_copy(b):
        span = pl.ds(b * SLOTS, SLOTS)
        return pltpu.make_async_copy(prompts.at[span], prompt_buf.at[span], prompt_sem.at[b])

    def partners(i):
        return [3 - i, lax.rem(i + 2, 4), i + 1 - 2 * lax.rem(i, 2)]

    seq_peers = partners(me)
    tensor_peers = [lax.rem(mine + 2, 4), 3 - mine, mine + 1 - 2 * lax.rem(mine, 2)]

    w_rows = w_out.shape[0] // 2

    def w_copy(k, i):
        column = tensor_peers[k] if k < 3 else mine
        start = pl.multiple_of(column * cols, 128)
        span = pl.ds(i * w_rows, w_rows)
        return pltpu.make_async_copy(
            w_out.at[span, pl.ds(start, cols)], w_buf.at[k, span], w_sem.at[2 * k + i]
        )

    for copy in smalls:
        copy.start()

    def start_all(count, start_one):
        def one(i, carry):
            start_one(i)
            return carry

        lax.fori_loop(0, count, one, 0)

    for n in range(2):
        start_all(steps, lambda c, n=n: q_copy(n, c).start())
    start_all(pages // SLOTS, lambda b: pool_copy(b).start())
    start_all(n_tasks // SLOTS, lambda b: prompt_copy(b).start())
    start_all(steps, lambda c: kv_copy(w_key, k_buf, k_sem, c).start())
    start_all(steps, lambda c: kv_copy(w_value, v_buf, v_sem, c).start())
    for k in range(4):
        start_all(2, lambda i, k=k: w_copy(k, i).start())

    barrier = pltpu.get_barrier_semaphore()
    for peer in seq_peers:
        pl.semaphore_signal(barrier, inc=1, device_id={"seq": peer}, device_id_type=MESH)
    for peer in tensor_peers:
        pl.semaphore_signal(barrier, inc=1, device_id={"tensor": peer}, device_id_type=MESH)

    qwide[...] = jnp.zeros_like(qwide)
    for copy in smalls:
        copy.wait()
    x = hidden[...].astype(jnp.float32)
    mean_square = jnp.mean(x * x, axis=-1, keepdims=True)
    normed[...] = (x * lax.rsqrt(mean_square + 1e-06) * pre_gain[...][None]).astype(jnp.bfloat16)

    row = lax.broadcasted_iota(jnp.int32, (rows, requests), 0)
    column = lax.broadcasted_iota(jnp.int32, (rows, requests), 1)
    own_length = jnp.sum(
        jnp.where(column == me * rows + row, lengths[...].astype(jnp.float32), 0.0),
        axis=1, keepdims=True,
    )
    angles = (own_length + prompt_len) * frequency[...]
    lane = lax.broadcasted_iota(jnp.int32, (rows, hd), 1)
    cos_all = jnp.cos(angles)
    sin_all = jnp.sin(angles)
    sin_all = jnp.where(lane < hd // 2, -sin_all, sin_all)

    query_copies = []
    for n in range(2):
        lanes = slice(n * half, (n + 1) * half)
        acc = None
        for c in range(steps):
            q_copy(n, c).wait()
            term = jnp.dot(
                normed[:, c * chunk : (c + 1) * chunk],
                q_buf[c * chunk : (c + 1) * chunk, lanes],
                preferred_element_type=jnp.float32,
            )
            acc = term if acc is None else acc + term
        turned = jnp.concatenate(
            [
                rope_lanes(acc[:, i * hd : (i + 1) * hd], cos_all, sin_all)
                for i in range(half // hd)
            ],
            axis=1,
        ).astype(jnp.bfloat16)
        queries[pl.ds(me, 1), :, lanes] = turned[None]
        if n == 0:
            pl.semaphore_wait(barrier, 6)
        for k, peer in enumerate(seq_peers):
            where = queries.at[me, :, pl.ds(n * half, half)]
            copy = pltpu.make_async_remote_copy(
                src_ref=where, dst_ref=where,
                send_sem=query_send.at[n * 3 + k], recv_sem=query_recv.at[n * 3 + k],
                device_id={"seq": peer}, device_id_type=MESH,
            )
            copy.start()
            query_copies.append(copy)

    page_id = me * pages + lax.broadcasted_iota(jnp.int32, (pages, requests), 0)

    def match_one(j, carry):
        hot, count = carry
        hit = jnp.broadcast_to(table[pl.ds(j, 1), :], (pages, requests)) == page_id
        tokens = jnp.broadcast_to(
            jnp.clip(lengths[...] - j * block_len, 0, block_len), (pages, requests)
        )
        return jnp.where(hit, 1.0, hot), jnp.where(hit, tokens.astype(jnp.float32), count)

    zeros = jnp.zeros((pages, requests), jnp.float32)
    hot, count = lax.fori_loop(0, max_blocks, match_one, (zeros, zeros))
    onehot[...] = hot.astype(jnp.bfloat16)
    turned = hot.T.astype(jnp.bfloat16)
    onehot_t[...] = jnp.concatenate([turned, turned], axis=1)
    valid[...] = jnp.broadcast_to(jnp.sum(count, axis=1, keepdims=True), valid.shape)
    line = lax.broadcasted_iota(jnp.int32, (requests, requests), 0)
    across = lax.broadcasted_iota(jnp.int32, (requests, requests), 1)
    local = tasks_row[...] - me * n_tasks
    is_owned = jnp.where((local >= 0) & (local < n_tasks), 1.0, 0.0)
    owned[...] = jnp.broadcast_to(
        jnp.sum(jnp.where(line == across, is_owned, 0.0), axis=1, keepdims=True), owned.shape
    )

    sizes = (heads, kv_heads, hd, score_scale)
    tiles = kv_width // 256
    tile_heads = heads // tiles
    token = lax.broadcasted_iota(jnp.int32, (SLOTS, TOKENS), 1)
    per = TOKENS // prompt_len
    slot_of = lax.broadcasted_iota(jnp.int32, (SLOTS, TOKENS), 0)
    fits = token // prompt_len == slot_of % per
    pool_groups = pages // SLOTS
    halves = rows // SLOTS
    takers = seq_peers + [me]

    def widen(slot, t, source):
        for h in range(t * tile_heads, (t + 1) * tile_heads):
            kv = h // group
            qwide[slot, h * SLOTS : (h + 1) * SLOTS, kv * hd : (kv + 1) * hd] = source(
                slice(h * hd, (h + 1) * hd)
            )

    def pool_group(g):
        start = g * SLOTS

        def load(which):
            def one(pair, t):
                first = start + 2 * pair
                return pool_buf[first : first + 2, which, :, t * 256 : (t + 1) * 256].reshape(
                    2 * block_len, 256
                )

            return one

        live = jnp.where(token.astype(jnp.float32) < valid[start : start + SLOTS, :], 1.0, 0.0)
        return (qwide.at[g % 4], load(0), load(1), SLOTS // 2, 1, live)

    def pool_scores(made, g, t):
        widen(g % 4, t, lambda lanes: page_query[g * SLOTS : (g + 1) * SLOTS, lanes])
        return tile_scores(sizes, t, *made)

    def prompt_group(n):
        peer, s = takers[n // halves], n % halves
        first = peer * rows + s * SLOTS
        places = [
            jnp.clip(tasks[first + i] - me * n_tasks, 0, n_tasks - 1) for i in range(SLOTS)
        ]

        def load(which):
            def one(pair, t):
                return jnp.concatenate(
                    [
                        prompt_buf[place, which, :, t * 256 : (t + 1) * 256]
                        for place in places[pair * 2 * per : (pair + 1) * 2 * per]
                    ],
                    axis=0,
                )

            return one

        start = pl.multiple_of(first, SLOTS)
        live = jnp.where(fits, owned[pl.ds(start, SLOTS), :], 0.0)
        return (qwide.at[n % 4], load(0), load(1), SLOTS // (2 * per), per, live)

    def prompt_scores(made, n):
        peer, s = takers[n // halves], n % halves
        scores = []
        for t in range(tiles):
            widen(n % 4, t, lambda lanes: queries[peer, s * SLOTS : (s + 1) * SLOTS, lanes])
            scores.append(tile_scores(sizes, t, *made))
        return scores

    def finish_pool(g, made, scores):
        for i, piece in enumerate(group_mixes(sizes, scores, made)):
            page_mix[g * SLOTS : (g + 1) * SLOTS, i * hd : (i + 1) * hd] = piece

    mix_copies = []

    def finish_prompt(n, made, scores):
        k, s = n // halves, n % halves
        peer = takers[k]
        span = slice(s * SLOTS, (s + 1) * SLOTS)
        start = pl.multiple_of(peer * rows + s * SLOTS, SLOTS)
        for i, piece in enumerate(group_mixes(sizes, scores, made)):
            lanes = slice(i * hd, (i + 1) * hd)
            sums = req_mix[pl.ds(start, SLOTS), lanes] + piece
            if k < 3:
                packed[k, span, lanes] = sums.astype(jnp.bfloat16)
            else:
                req_mix[pl.ds(start, SLOTS), lanes] = sums
        if k < 3:
            copy = pltpu.make_async_remote_copy(
                src_ref=packed.at[k, span], dst_ref=landed.at[k, span],
                send_sem=mix_send.at[n], recv_sem=mix_recv.at[n],
                device_id={"seq": peer}, device_id_type=MESH,
            )
            copy.start()
            mix_copies.append(copy)

    pools = [pool_group(g) for g in range(pool_groups)]
    early = 2
    scores = [[] for _ in pools]
    for t in range(tiles):
        for copy in query_copies[3 * t : 3 * (t + 1)]:
            copy.wait()
        lanes = slice(t * half, (t + 1) * half)
        page_query[:, lanes] = jnp.dot(
            onehot[...], queries[:, :, lanes].reshape(requests, half),
            preferred_element_type=jnp.float32,
        ).astype(jnp.bfloat16)
        if t == 0:
            for g in range(early):
                pool_copy(g).wait()
                scores[g].append(pool_scores(pools[g], g, t))
    for g in range(pool_groups):
        if g >= early:
            pool_copy(g).wait()
        for t in range(len(scores[g]), tiles):
            scores[g].append(pool_scores(pools[g], g, t))
        if g:
            finish_pool(g - 1, pools[g - 1], scores[g - 1])
    finish_pool(pool_groups - 1, pools[-1], scores[-1])
    high = page_mix[...].astype(jnp.bfloat16)
    both[:pages, :] = high
    both[pages:, :] = (page_mix[...] - high.astype(jnp.float32)).astype(jnp.bfloat16)
    req_mix[...] = jnp.dot(onehot_t[...], both[...], preferred_element_type=jnp.float32)
    for b in range(n_tasks // SLOTS):
        prompt_copy(b).wait()
    made = prompt_group(0)
    ahead = (made, prompt_scores(made, 0))
    for n in range(1, len(takers) * halves):
        made = prompt_group(n)
        later = (made, prompt_scores(made, n))
        finish_prompt(n - 1, *ahead)
        ahead = later
    finish_prompt(len(takers) * halves - 1, *ahead)

    def kv_product(src, dst, sem):
        acc = None
        for c in range(steps):
            kv_copy(src, dst, sem, c).wait()
            term = jnp.dot(
                normed[:, c * chunk : (c + 1) * chunk],
                dst[c * chunk : (c + 1) * chunk, :],
                preferred_element_type=jnp.float32,
            )
            acc = term if acc is None else acc + term
        return acc

    key_new = kv_product(w_key, k_buf, k_sem)
    for g in range(kv_heads):
        lanes = slice(g * hd, (g + 1) * hd)
        fresh[0, :, lanes] = rope_lanes(key_new[:, lanes], cos_all, sin_all).astype(jnp.bfloat16)
    self_weights = []
    for h in range(heads):
        g = h // group
        q = queries[me, :, h * hd : (h + 1) * hd].astype(jnp.float32)
        k = fresh[0, :, g * hd : (g + 1) * hd].astype(jnp.float32)
        raw = jnp.sum(q * k, axis=1, keepdims=True)
        self_weights.append(jnp.exp(cap_limit * jnp.tanh(raw * (score_scale / cap_limit))))
    fresh[1] = kv_product(w_value, v_buf, v_sem).astype(jnp.bfloat16)
    for i in range(2):
        fresh_rows[:, i, :] = fresh[i].astype(jnp.float32)
    fresh_out[...] = fresh_rows[...].astype(jnp.bfloat16)
    for copy in mix_copies:
        copy.wait()
    own = pl.ds(pl.multiple_of(me * rows, SLOTS), rows)
    totals = req_mix[own, q_width:]
    for k in range(3):
        totals += landed[k, :, q_width:].astype(jnp.float32)
    for h in range(heads):
        g = h // group
        lanes = slice(h * hd, (h + 1) * hd)
        mix = req_mix[own, lanes]
        for k in range(3):
            mix += landed[k, :, lanes].astype(jnp.float32)
        total = totals[:, h : h + 1] + self_weights[h]
        rounded = self_weights[h].astype(jnp.bfloat16).astype(jnp.float32)
        mix += rounded * fresh[1, :, g * hd : (g + 1) * hd].astype(jnp.float32)
        attended[:, lanes] = (mix / total).astype(jnp.bfloat16)

    is_inner = lax.rem(mine, 3) != 0
    onward = lax.rem(2 * mine + 1, 5)
    pieces = (slice(0, cut), slice(cut, cols))

    def project(k, piece):
        return jnp.dot(attended[...], w_buf[k, :, piece], preferred_element_type=jnp.float32)

    def part(i, k, piece, peer):
        return pltpu.make_async_remote_copy(
            src_ref=sent.at[k, :, piece], dst_ref=arrived.at[k, :, piece],
            send_sem=part_send.at[i], recv_sem=part_recv.at[i],
            device_id={"tensor": peer}, device_id_type=MESH,
        )

    handed = [part(i, 0, pieces[i], onward) for i in range(2)]
    mirrored = [part(2 + i, 1, pieces[i], tensor_peers[1]) for i in range(2)]
    beside = part(4, 2, slice(0, cols), tensor_peers[2])
    for i in range(2):
        w_copy(0, i).wait()
    for piece, copy in zip(pieces, handed):
        sent[0, :, piece] = project(0, piece).astype(jnp.bfloat16)
        copy.start()
    for i in range(2):
        w_copy(1, i).wait()
    for piece, copy in zip(pieces, mirrored):
        held[:, piece] = project(1, piece)

        @pl.when(jnp.logical_not(is_inner))
        def _():
            sent[1, :, piece] = held[:, piece].astype(jnp.bfloat16)
            copy.start()

    for i in range(2):
        w_copy(2, i).wait()
    sent[2] = project(2, slice(0, cols)).astype(jnp.bfloat16)
    beside.start()
    for i in range(2):
        w_copy(3, i).wait()
    whole_sum[...] = project(3, slice(0, cols))
    for piece, take, copy in zip(pieces, handed, mirrored):

        @pl.when(is_inner)
        def _():
            take.wait_recv()
            total = held[:, piece] + arrived[0, :, piece].astype(jnp.float32)
            sent[1, :, piece] = total.astype(jnp.bfloat16)
            copy.start()

    beside.wait_recv()
    whole_sum[...] += arrived[2].astype(jnp.float32)

    @pl.when(jnp.logical_not(is_inner))
    def _():
        for copy in handed:
            copy.wait_recv()
        whole_sum[...] += arrived[0].astype(jnp.float32)

    for copy in mirrored:
        copy.wait_recv()
    whole = whole_sum[...] + arrived[1].astype(jnp.float32)
    part_square = jnp.sum(whole * whole, axis=1, keepdims=True)
    row = lax.broadcasted_iota(jnp.int32, (rows, 128), 0)
    diagonal = row == lax.broadcasted_iota(jnp.int32, (rows, 128), 1)
    square[...] = jnp.sum(jnp.where(diagonal, part_square, 0.0), axis=0, keepdims=True)
    copies = []
    for k, peer in enumerate(tensor_peers):
        copy = pltpu.make_async_remote_copy(
            src_ref=square, dst_ref=squares.at[k],
            send_sem=square_send.at[k], recv_sem=square_recv.at[k],
            device_id={"tensor": peer}, device_id_type=MESH,
        )
        copy.start()
        copies.append(copy)
    scaled = whole * post_gain[...][None]
    start = pl.multiple_of(mine * cols, 128)
    residual = hidden[:, pl.ds(start, cols)].astype(jnp.float32)
    for copy in copies:
        copy.wait()
    total_square = square[...]
    for k in range(3):
        total_square += squares[k]
    column_square = jnp.sum(jnp.where(diagonal, total_square, 0.0), axis=1, keepdims=True)
    factor = lax.rsqrt(column_square / (cols * tensor) + 1e-06)
    out[...] = (residual + scaled * factor).astype(jnp.bfloat16)
    for copy in handed + mirrored + [beside]:
        copy.wait_send()


STEPS = 3


def place_kernel(layer_in, fresh_in, layer_out, fresh_out, sems):
    copies = [
        pltpu.make_async_copy(layer_in, layer_out, sems.at[0]),
        pltpu.make_async_copy(fresh_in, fresh_out, sems.at[1]),
    ]
    for copy in copies:
        copy.start()
    for copy in copies:
        copy.wait()


def body(
    seq, tensor, hidden, pre_gain, w_query, w_key, w_value, w_out, post_gain,
    cache_pool, prompt_cache, task_ids, cache_lengths, block_table,
):
    rows, depth = hidden.shape
    requests = task_ids.shape[0]
    pages, _, _, kv_width = cache_pool.shape
    n_tasks = prompt_cache.shape[0]
    q_width = w_query.shape[1]
    heads = q_width // HD
    cols = post_gain.shape[0]
    score_scale = float(D // H) ** (-0.5)
    half = HD // 2
    frequency = 10000.0 ** (-np.arange(half) / half)
    frequency = jnp.asarray(np.concatenate([frequency, frequency])[None], jnp.float32)
    vmem = pl.BlockSpec(memory_space=pltpu.VMEM)
    hbm = pl.BlockSpec(memory_space=pl.ANY)
    dma = pltpu.SemaphoreType.DMA
    bf16, f32, i32 = jnp.bfloat16, jnp.float32, jnp.int32
    packed_width = q_width + HD
    layer_out, fresh = pl.pallas_call(
        functools.partial(layer_kernel, seq, tensor, score_scale, HD, STEPS),
        out_shape=(
            pltpu.VMEM((rows, cols), bf16),
            pltpu.VMEM((rows, 2, kv_width), bf16),
        ),
        in_specs=[hbm] * 14,
        out_specs=(vmem, vmem),
        scratch_shapes=[
            pltpu.VMEM((1, requests), i32),
            pltpu.SMEM((requests,), i32),
            pltpu.VMEM((1, requests), i32),
            pltpu.VMEM((block_table.shape[1], requests), i32),
            pltpu.VMEM((rows, depth), bf16),
            pltpu.VMEM((depth,), f32),
            pltpu.VMEM((1, HD), f32),
            pltpu.VMEM((cols,), f32),
            pltpu.VMEM((rows, depth), bf16),
            pltpu.VMEM((seq, rows, q_width), bf16),
            pltpu.VMEM((depth, q_width), bf16),
            pltpu.VMEM((depth, kv_width), bf16),
            pltpu.VMEM((depth, kv_width), bf16),
            pltpu.VMEM((tensor, w_out.shape[0], cols), bf16),
            pltpu.VMEM(cache_pool.shape, bf16),
            pltpu.VMEM(prompt_cache.shape, bf16),
            pltpu.VMEM((pages, requests), bf16),
            pltpu.VMEM((requests, 2 * pages), bf16),
            pltpu.VMEM((pages, TOKENS), f32),
            pltpu.VMEM((requests, TOKENS), f32),
            pltpu.VMEM((pages, q_width), bf16),
            pltpu.VMEM((4, heads * SLOTS, kv_width), bf16),
            pltpu.VMEM((pages, packed_width), f32),
            pltpu.VMEM((2 * pages, packed_width), bf16),
            pltpu.VMEM((requests, packed_width), f32),
            pltpu.VMEM((3, rows, packed_width), bf16),
            pltpu.VMEM((3, rows, packed_width), bf16),
            pltpu.VMEM((2, rows, kv_width), bf16),
            pltpu.VMEM((rows, 2, kv_width), f32),
            pltpu.VMEM((rows, q_width), bf16),
            pltpu.VMEM((3, rows, cols), bf16),
            pltpu.VMEM((3, rows, cols), bf16),
            pltpu.VMEM((rows, cols), f32),
            pltpu.VMEM((rows, cols), f32),
            pltpu.VMEM((1, 128), f32),
            pltpu.VMEM((3, 1, 128), f32),
            dma((8,)),
            dma((2 * STEPS,)),
            dma((STEPS,)),
            dma((STEPS,)),
            dma((2 * tensor,)),
            dma((pages // SLOTS,)),
            dma((n_tasks // SLOTS,)),
            dma((6,)),
            dma((6,)),
            dma((6,)),
            dma((6,)),
            dma((5,)),
            dma((5,)),
            dma((3,)),
            dma((3,)),
        ],
        compiler_params=pltpu.CompilerParams(
            collective_id=0, has_side_effects=True, vmem_limit_bytes=VMEM_BYTES
        ),
    )(
        cache_lengths.reshape(1, -1), task_ids, task_ids.reshape(1, -1), block_table.T,
        hidden, pre_gain, frequency, post_gain,
        w_query, w_key, w_value, w_out, cache_pool, prompt_cache,
    )
    return pl.pallas_call(
        place_kernel,
        out_shape=(
            jax.ShapeDtypeStruct((rows, cols), bf16),
            jax.ShapeDtypeStruct((rows, 2, kv_width), bf16),
        ),
        in_specs=[vmem, vmem],
        out_specs=(hbm, hbm),
        scratch_shapes=[dma((2,))],
        compiler_params=pltpu.CompilerParams(vmem_limit_bytes=1024 * 1024),
    )(layer_out, fresh)


def fits(seq, tensor, arrays):
    hidden, w_query, w_key, post_gain = arrays[0], arrays[2], arrays[3], arrays[6]
    pool, prompts, tasks = arrays[7], arrays[8], arrays[9]
    return (
        seq == 4
        and tensor == 4
        and hidden.shape[0] == 2 * SLOTS
        and hidden.shape[1] % (STEPS * 256) == 0
        and w_query.shape[1] == 8 * HD
        and w_key.shape[1] == 4 * HD
        and post_gain.shape[0] % 128 == 0
        and pool.shape[0] == 64
        and pool.shape[2] == TOKENS
        and prompts.shape[0] % SLOTS == 0
        and prompts.shape[2] == TOKENS // 2
        and tasks.shape[0] == 128
    )


def solution(mesh):
    seq, tensor = mesh.shape["seq"], mesh.shape["tensor"]

    def chosen(*arrays):
        if not fits(seq, tensor, arrays):
            return plain_body(*arrays)
        return body(seq, tensor, *arrays)

    return jax.shard_map(
        chosen,
        mesh=mesh,
        in_specs=(
            P(("groups", "seq"), None),
            P(),
            P(None, "tensor"),
            P(None, "tensor"),
            P(None, "tensor"),
            P("tensor", None),
            P("tensor"),
            P(("groups", "seq"), None, None, "tensor"),
            P("seq", None, None, "tensor"),
            P("groups"),
            P("groups"),
            P("groups", None),
        ),
        out_specs=(P(("groups", "seq"), "tensor"), P(("groups", "seq"), None, "tensor")),
        check_vma=False,
    )
```

```python
import jax
import jax.numpy as jnp
from jax import lax
from jax.experimental import pallas as pl
from jax.experimental.pallas import tpu as pltpu
from jax.sharding import PartitionSpec as P
import functools
import numpy as np

D = 4608
H = 32
HD = 128


cap_limit = 50.0


def rms_scale(values, gain):
    mean_square = jnp.mean(values * values, axis=-1, keepdims=True)
    return values * lax.rsqrt(mean_square + 1e-06) * gain


def rotate(values, position):
    half_dim = values.shape[-1] // 2
    frequency = 10000.0 ** (-jnp.arange(half_dim, dtype=jnp.float32) / half_dim)
    angles = position.astype(jnp.float32)[:, None] * frequency[None, :]
    cosine = jnp.cos(angles)[:, None, :]
    sines = jnp.sin(angles)[:, None, :]
    first_half = values[..., :half_dim]
    second_half = values[..., half_dim:]
    return jnp.concatenate(
        [first_half * cosine - second_half * sines, second_half * cosine + first_half * sines],
        axis=-1,
    )


def capped(raw_score, score_scale):
    return cap_limit * jnp.tanh(raw_score * score_scale / cap_limit)


def attend(query_block, block, live_mask, score_scale):
    count = block.shape[0]
    length = block.shape[2]
    kv_heads = query_block.shape[1]
    head_dim = query_block.shape[3]
    block_keys = block[:, 0].reshape(count, length, kv_heads, head_dim)
    block_values = block[:, 1].reshape(count, length, kv_heads, head_dim)
    raw_score = jnp.einsum(
        "nkgd,ntkd->nkgt", query_block, block_keys, preferred_element_type=jnp.float32
    )
    weight = jnp.where(live_mask[:, None, None, :], jnp.exp(capped(raw_score, score_scale)), 0.0)
    totals = jnp.sum(weight, axis=-1).reshape(count, -1)
    mixtures = jnp.einsum(
        "nkgt,ntkd->nkgd",
        weight.astype(jnp.bfloat16),
        block_values,
        preferred_element_type=jnp.float32,
    )
    return (totals, mixtures.reshape(count, -1))


def plain_body(
    hidden,
    pre_gain,
    w_query,
    w_key,
    w_value,
    w_out,
    post_gain,
    cache_pool,
    prompt_cache,
    task_ids,
    cache_lengths,
    block_table,
):
    seq_index = lax.axis_index("seq")
    tensor_index = lax.axis_index("tensor")
    own_rows = hidden.shape[0]
    requests = task_ids.shape[0]
    pages_dev = cache_pool.shape[0]
    block_len = cache_pool.shape[2]
    kv_width = cache_pool.shape[3]
    head_dim = HD
    kv_heads = kv_width // head_dim
    query_heads = w_query.shape[1] // head_dim
    group_size = query_heads // kv_heads
    prompt_len = prompt_cache.shape[2]
    tasks_dev = prompt_cache.shape[0]
    score_scale = float(D // H) ** (-0.5)
    first_row = seq_index * own_rows
    own_lengths = lax.dynamic_slice_in_dim(cache_lengths, first_row, own_rows)
    normed = rms_scale(hidden.astype(jnp.float32), pre_gain).astype(jnp.bfloat16)
    position = prompt_len + own_lengths
    query_rows = rotate(
        jnp.dot(normed, w_query, preferred_element_type=jnp.float32).reshape(
            own_rows, query_heads, head_dim
        ),
        position,
    ).astype(jnp.bfloat16)
    key_new = rotate(
        jnp.dot(normed, w_key, preferred_element_type=jnp.float32).reshape(
            own_rows, kv_heads, head_dim
        ),
        position,
    ).astype(jnp.bfloat16)
    value_new = jnp.dot(normed, w_value, preferred_element_type=jnp.float32).astype(jnp.bfloat16)
    fresh_cache = jnp.stack([key_new.reshape(own_rows, kv_width), value_new], axis=1)
    queries = lax.all_gather(
        query_rows.reshape(own_rows, query_heads * head_dim), "seq", axis=0, tiled=True
    )
    page_ids = seq_index * pages_dev + jnp.arange(pages_dev)
    flat_table = block_table.reshape(-1)
    max_blocks = block_table.shape[1]
    matches = flat_table[None, :] == page_ids[:, None]
    entry_index = jnp.arange(flat_table.shape[0])
    page_used = jnp.any(matches, axis=1)
    found_entry = jnp.sum(jnp.where(matches, entry_index[None, :], 0), axis=1)
    page_owner = found_entry // max_blocks
    block_number = found_entry % max_blocks
    owner_hot = (page_owner[:, None] == jnp.arange(requests)[None, :]) & page_used[:, None]
    owner_length = jnp.sum(jnp.where(owner_hot, cache_lengths[None, :], 0), axis=1)
    valid_count = jnp.clip(owner_length - block_number * block_len, 0, block_len)
    page_query = jnp.dot(
        owner_hot.astype(jnp.bfloat16), queries, preferred_element_type=jnp.float32
    ).astype(jnp.bfloat16)
    page_query = page_query.reshape(pages_dev, kv_heads, group_size, head_dim)
    page_live = jnp.arange(block_len)[None, :] < valid_count[:, None]
    page_totals, page_mixtures = attend(page_query, cache_pool, page_live, score_scale)
    spread_hot = owner_hot.astype(jnp.float32).T
    totals = jnp.dot(spread_hot, page_totals, precision=lax.Precision.HIGHEST)
    mixtures = jnp.dot(spread_hot, page_mixtures, precision=lax.Precision.HIGHEST)
    local_task = task_ids - seq_index * tasks_dev
    is_owned = (local_task >= 0) & (local_task < tasks_dev)
    task_rows = prompt_cache[jnp.clip(local_task, 0, tasks_dev - 1)]
    all_query = queries.reshape(requests, kv_heads, group_size, head_dim)
    owned_live = jnp.broadcast_to(is_owned[:, None], (requests, prompt_len))
    prompt_totals, prompt_mixtures = attend(all_query, task_rows, owned_live, score_scale)
    totals = totals + prompt_totals
    mixtures = mixtures + prompt_mixtures
    totals, mixtures = (
        lax.psum_scatter(
            totals.astype(jnp.bfloat16), "seq", scatter_dimension=0, tiled=True
        ).astype(jnp.float32),
        lax.psum_scatter(
            mixtures.astype(jnp.bfloat16), "seq", scatter_dimension=0, tiled=True
        ).astype(jnp.float32),
    )
    own_query = query_rows.reshape(own_rows, kv_heads, group_size, head_dim)
    self_raw = jnp.sum(
        own_query.astype(jnp.float32) * key_new[:, :, None, :].astype(jnp.float32), axis=-1
    )
    self_weight = jnp.exp(capped(self_raw, score_scale))
    rounded = lax.optimization_barrier(self_weight.astype(jnp.bfloat16)).astype(jnp.float32)
    totals = totals + self_weight.reshape(own_rows, -1)
    self_mix = rounded[..., None] * value_new.reshape(own_rows, kv_heads, 1, head_dim).astype(
        jnp.float32
    )
    mixtures = mixtures + self_mix.reshape(own_rows, -1)
    attended = (mixtures.reshape(own_rows, query_heads, head_dim) / totals[..., None]).astype(
        jnp.bfloat16
    )
    projected = jnp.dot(
        attended.reshape(own_rows, query_heads * head_dim),
        w_out,
        preferred_element_type=jnp.float32,
    )
    cols_local = post_gain.shape[0]
    col_start = tensor_index * cols_local
    residual = lax.dynamic_slice_in_dim(hidden, col_start, cols_local, 1).astype(jnp.float32)
    whole_sum = lax.psum(projected.astype(jnp.bfloat16), "tensor").astype(jnp.float32)
    mean_square = jnp.mean(whole_sum * whole_sum, axis=1, keepdims=True)
    scaled = lax.dynamic_slice_in_dim(whole_sum, col_start, cols_local, 1) * lax.rsqrt(
        mean_square + 1e-06
    )
    layer_out = (residual + scaled * post_gain).astype(jnp.bfloat16)
    return (layer_out, fresh_cache)


MESH = pl.DeviceIdType.MESH
VMEM_BYTES = 62 * 1024 * 1024


def rope_lanes(x, cosine, sines):
    return x * cosine + pltpu.roll(x, x.shape[-1] // 2, 1) * sines


SLOTS = 16
TOKENS = 128


def stacked(x, count):
    return jnp.concatenate([x] * count, axis=0)


def slot_unit(per):
    return lax.broadcasted_iota(jnp.int32, (SLOTS, TOKENS), 0) // per


def tile_scores(sizes, t, qwide, keys, values, pairs, per, live):
    heads, kv_heads, hd, score_scale = sizes
    tile_heads = heads * 256 // (kv_heads * hd)
    rows = tile_heads * SLOTS
    unit = stacked(slot_unit(per), tile_heads)
    across = lax.broadcasted_iota(jnp.int32, (TOKENS, rows), 1) % SLOTS // per
    q = qwide[t * rows : (t + 1) * rows, t * 256 : (t + 1) * 256]
    held, streamed = None, None
    for pair in range(pairs):
        two = (keys(pair, t), q) if pair % 2 == 0 else (q, keys(pair, t))
        raw = lax.dot_general(
            *two, (((1,), (1,)), ((), ())), preferred_element_type=jnp.float32
        )
        for u in range(2):
            if pair % 2 == 0:
                part = raw[u * TOKENS : (u + 1) * TOKENS]
                streamed = part if streamed is None else jnp.where(
                    across == 2 * pair + u, part, streamed
                )
            else:
                part = raw[:, u * TOKENS : (u + 1) * TOKENS]
                held = part if held is None else jnp.where(unit == 2 * pair + u, part, held)
    return jnp.where(unit // 2 % 2 == 0, streamed.T, held)


def tile_mixes(sizes, chosen, t, qwide, keys, values, pairs, per, live):
    heads, kv_heads, hd, score_scale = sizes
    tile_heads = heads * 256 // (kv_heads * hd)
    weight = jnp.exp(cap_limit * jnp.tanh(chosen * (score_scale / cap_limit)))
    weight = jnp.where(stacked(live, tile_heads) > 0, weight, 0.0)
    total = jnp.sum(weight, axis=1, keepdims=True)
    narrow = weight.astype(jnp.bfloat16)
    acc = None
    for pair in range(pairs):
        pieces = []
        for u in range(2):
            keep = (slot_unit(per) == 2 * pair + u).astype(jnp.float32).astype(jnp.bfloat16)
            pieces.append(narrow * stacked(keep, tile_heads))
        term = jnp.dot(
            jnp.concatenate(pieces, axis=1), values(pair, t), preferred_element_type=jnp.float32
        )
        acc = term if acc is None else acc + term
    mixes, totals = [], []
    for i in range(tile_heads):
        span = slice(i * SLOTS, (i + 1) * SLOTS)
        kv = i // (heads // kv_heads)
        mixes.append(acc[span, kv * hd : (kv + 1) * hd])
        totals.append(total[span])
    return mixes, totals


def group_mixes(sizes, scores, group):
    heads, hd = sizes[0], sizes[2]
    mixes, totals = [], []
    for t, chosen in enumerate(scores):
        more = tile_mixes(sizes, chosen, t, *group)
        mixes += more[0]
        totals += more[1]
    lane = lax.broadcasted_iota(jnp.int32, (SLOTS, hd), 1)
    packed_total = jnp.zeros((SLOTS, hd), jnp.float32)
    for h in range(heads):
        packed_total = jnp.where(lane == h, totals[h], packed_total)
    return mixes + [packed_total]


def layer_kernel(
    seq, tensor, score_scale, hd, steps,
    lengths_in, tasks_in, tasks_row_in, table_in, hidden_in, pre_gain_in, frequency_in, post_gain_in,
    w_query, w_key, w_value, w_out, pool, prompts,
    out, fresh_out,
    lengths, tasks, tasks_row, table, hidden, pre_gain, frequency, post_gain,
    normed, queries, q_buf, k_buf, v_buf, w_buf, pool_buf, prompt_buf,
    onehot, onehot_t, valid, owned, page_query, qwide, page_mix, both, req_mix, packed, landed,
    fresh, fresh_rows, attended, sent, arrived, held, whole_sum, square, squares,
    small_sem, q_sem, k_sem, v_sem, w_sem, pool_sem, prompt_sem,
    query_send, query_recv, mix_send, mix_recv, part_send, part_recv, square_send, square_recv,
):
    me = lax.axis_index("seq")
    mine = lax.axis_index("tensor")
    rows, depth = hidden.shape
    cols = out.shape[1]
    requests = lengths.shape[1]
    q_width = q_buf.shape[1]
    kv_width = k_buf.shape[1]
    heads, kv_heads = q_width // hd, kv_width // hd
    group = heads // kv_heads
    pages, _, block_len, _ = pool.shape
    n_tasks, _, prompt_len, _ = prompts.shape
    max_blocks = table.shape[0]
    half = q_width // 2
    chunk = depth // steps
    cut = cols // 256 * 128

    smalls = []
    for i, (src, dst) in enumerate((
        (hidden_in, hidden), (pre_gain_in, pre_gain), (frequency_in, frequency),
        (lengths_in, lengths), (tasks_in, tasks), (tasks_row_in, tasks_row),
        (table_in, table), (post_gain_in, post_gain),
    )):
        smalls.append(pltpu.make_async_copy(src, dst, small_sem.at[i]))

    def q_copy(n, c):
        span, lanes = pl.ds(c * chunk, chunk), pl.ds(n * half, half)
        return pltpu.make_async_copy(
            w_query.at[span, lanes], q_buf.at[span, lanes], q_sem.at[n * steps + c]
        )

    def kv_copy(src, dst, sem, c):
        span = pl.ds(c * chunk, chunk)
        return pltpu.make_async_copy(src.at[span], dst.at[span], sem.at[c])

    def pool_copy(b):
        span = pl.ds(b * SLOTS, SLOTS)
        return pltpu.make_async_copy(pool.at[span], pool_buf.at[span], pool_sem.at[b])

    def prompt_copy(b):
        span = pl.ds(b * SLOTS, SLOTS)
        return pltpu.make_async_copy(prompts.at[span], prompt_buf.at[span], prompt_sem.at[b])

    def partners(i):
        return [3 - i, lax.rem(i + 2, 4), i + 1 - 2 * lax.rem(i, 2)]

    seq_peers = partners(me)
    tensor_peers = [lax.rem(mine + 2, 4), 3 - mine, mine + 1 - 2 * lax.rem(mine, 2)]

    w_rows = w_out.shape[0] // 2

    def w_copy(k, i):
        column = tensor_peers[k] if k < 3 else mine
        start = pl.multiple_of(column * cols, 128)
        span = pl.ds(i * w_rows, w_rows)
        return pltpu.make_async_copy(
            w_out.at[span, pl.ds(start, cols)], w_buf.at[k, span], w_sem.at[2 * k + i]
        )

    for copy in smalls:
        copy.start()

    def start_all(count, start_one):
        def one(i, carry):
            start_one(i)
            return carry

        lax.fori_loop(0, count, one, 0)

    for n in range(2):
        start_all(steps, lambda c, n=n: q_copy(n, c).start())
    start_all(pages // SLOTS, lambda b: pool_copy(b).start())
    start_all(n_tasks // SLOTS, lambda b: prompt_copy(b).start())
    start_all(steps, lambda c: kv_copy(w_key, k_buf, k_sem, c).start())
    start_all(steps, lambda c: kv_copy(w_value, v_buf, v_sem, c).start())
    for k in range(4):
        start_all(2, lambda i, k=k: w_copy(k, i).start())

    barrier = pltpu.get_barrier_semaphore()
    for peer in seq_peers:
        pl.semaphore_signal(barrier, inc=1, device_id={"seq": peer}, device_id_type=MESH)
    for peer in tensor_peers:
        pl.semaphore_signal(barrier, inc=1, device_id={"tensor": peer}, device_id_type=MESH)

    qwide[...] = jnp.zeros_like(qwide)
    for copy in smalls:
        copy.wait()
    x = hidden[...].astype(jnp.float32)
    mean_square = jnp.mean(x * x, axis=-1, keepdims=True)
    normed[...] = (x * lax.rsqrt(mean_square + 1e-06) * pre_gain[...][None]).astype(jnp.bfloat16)

    row = lax.broadcasted_iota(jnp.int32, (rows, requests), 0)
    column = lax.broadcasted_iota(jnp.int32, (rows, requests), 1)
    own_length = jnp.sum(
        jnp.where(column == me * rows + row, lengths[...].astype(jnp.float32), 0.0),
        axis=1, keepdims=True,
    )
    angles = (own_length + prompt_len) * frequency[...]
    lane = lax.broadcasted_iota(jnp.int32, (rows, hd), 1)
    cos_all = jnp.cos(angles)
    sin_all = jnp.sin(angles)
    sin_all = jnp.where(lane < hd // 2, -sin_all, sin_all)

    query_copies = []
    for n in range(2):
        lanes = slice(n * half, (n + 1) * half)
        acc = None
        for c in range(steps):
            q_copy(n, c).wait()
            term = jnp.dot(
                normed[:, c * chunk : (c + 1) * chunk],
                q_buf[c * chunk : (c + 1) * chunk, lanes],
                preferred_element_type=jnp.float32,
            )
            acc = term if acc is None else acc + term
        turned = jnp.concatenate(
            [
                rope_lanes(acc[:, i * hd : (i + 1) * hd], cos_all, sin_all)
                for i in range(half // hd)
            ],
            axis=1,
        ).astype(jnp.bfloat16)
        queries[pl.ds(me, 1), :, lanes] = turned[None]
        if n == 0:
            pl.semaphore_wait(barrier, 6)
        for k, peer in enumerate(seq_peers):
            where = queries.at[me, :, pl.ds(n * half, half)]
            copy = pltpu.make_async_remote_copy(
                src_ref=where, dst_ref=where,
                send_sem=query_send.at[n * 3 + k], recv_sem=query_recv.at[n * 3 + k],
                device_id={"seq": peer}, device_id_type=MESH,
            )
            copy.start()
            query_copies.append(copy)

    page_id = me * pages + lax.broadcasted_iota(jnp.int32, (pages, requests), 0)

    def match_one(j, carry):
        hot, count = carry
        hit = jnp.broadcast_to(table[pl.ds(j, 1), :], (pages, requests)) == page_id
        tokens = jnp.broadcast_to(
            jnp.clip(lengths[...] - j * block_len, 0, block_len), (pages, requests)
        )
        return jnp.where(hit, 1.0, hot), jnp.where(hit, tokens.astype(jnp.float32), count)

    zeros = jnp.zeros((pages, requests), jnp.float32)
    hot, count = lax.fori_loop(0, max_blocks, match_one, (zeros, zeros))
    onehot[...] = hot.astype(jnp.bfloat16)
    turned = hot.T.astype(jnp.bfloat16)
    onehot_t[...] = jnp.concatenate([turned, turned], axis=1)
    valid[...] = jnp.broadcast_to(jnp.sum(count, axis=1, keepdims=True), valid.shape)
    line = lax.broadcasted_iota(jnp.int32, (requests, requests), 0)
    across = lax.broadcasted_iota(jnp.int32, (requests, requests), 1)
    local = tasks_row[...] - me * n_tasks
    is_owned = jnp.where((local >= 0) & (local < n_tasks), 1.0, 0.0)
    owned[...] = jnp.broadcast_to(
        jnp.sum(jnp.where(line == across, is_owned, 0.0), axis=1, keepdims=True), owned.shape
    )

    sizes = (heads, kv_heads, hd, score_scale)
    tiles = kv_width // 256
    tile_heads = heads // tiles
    token = lax.broadcasted_iota(jnp.int32, (SLOTS, TOKENS), 1)
    per = TOKENS // prompt_len
    slot_of = lax.broadcasted_iota(jnp.int32, (SLOTS, TOKENS), 0)
    fits = token // prompt_len == slot_of % per
    pool_groups = pages // SLOTS
    halves = rows // SLOTS
    takers = seq_peers + [me]

    def widen(slot, t, source):
        for h in range(t * tile_heads, (t + 1) * tile_heads):
            kv = h // group
            qwide[slot, h * SLOTS : (h + 1) * SLOTS, kv * hd : (kv + 1) * hd] = source(
                slice(h * hd, (h + 1) * hd)
            )

    def pool_group(g):
        start = g * SLOTS

        def load(which):
            def one(pair, t):
                first = start + 2 * pair
                return pool_buf[first : first + 2, which, :, t * 256 : (t + 1) * 256].reshape(
                    2 * block_len, 256
                )

            return one

        live = jnp.where(token.astype(jnp.float32) < valid[start : start + SLOTS, :], 1.0, 0.0)
        return (qwide.at[g % 4], load(0), load(1), SLOTS // 2, 1, live)

    def pool_scores(made, g, t):
        widen(g % 4, t, lambda lanes: page_query[g * SLOTS : (g + 1) * SLOTS, lanes])
        return tile_scores(sizes, t, *made)

    def prompt_group(n):
        peer, s = takers[n // halves], n % halves
        first = peer * rows + s * SLOTS
        places = [
            jnp.clip(tasks[first + i] - me * n_tasks, 0, n_tasks - 1) for i in range(SLOTS)
        ]

        def load(which):
            def one(pair, t):
                return jnp.concatenate(
                    [
                        prompt_buf[place, which, :, t * 256 : (t + 1) * 256]
                        for place in places[pair * 2 * per : (pair + 1) * 2 * per]
                    ],
                    axis=0,
                )

            return one

        start = pl.multiple_of(first, SLOTS)
        live = jnp.where(fits, owned[pl.ds(start, SLOTS), :], 0.0)
        return (qwide.at[n % 4], load(0), load(1), SLOTS // (2 * per), per, live)

    def prompt_scores(made, n):
        peer, s = takers[n // halves], n % halves
        scores = []
        for t in range(tiles):
            widen(n % 4, t, lambda lanes: queries[peer, s * SLOTS : (s + 1) * SLOTS, lanes])
            scores.append(tile_scores(sizes, t, *made))
        return scores

    def finish_pool(g, made, scores):
        for i, piece in enumerate(group_mixes(sizes, scores, made)):
            page_mix[g * SLOTS : (g + 1) * SLOTS, i * hd : (i + 1) * hd] = piece

    mix_copies = []

    def finish_prompt(n, made, scores):
        k, s = n // halves, n % halves
        peer = takers[k]
        span = slice(s * SLOTS, (s + 1) * SLOTS)
        start = pl.multiple_of(peer * rows + s * SLOTS, SLOTS)
        for i, piece in enumerate(group_mixes(sizes, scores, made)):
            lanes = slice(i * hd, (i + 1) * hd)
            sums = req_mix[pl.ds(start, SLOTS), lanes] + piece
            if k < 3:
                packed[k, span, lanes] = sums.astype(jnp.bfloat16)
            else:
                req_mix[pl.ds(start, SLOTS), lanes] = sums
        if k < 3:
            copy = pltpu.make_async_remote_copy(
                src_ref=packed.at[k, span], dst_ref=landed.at[k, span],
                send_sem=mix_send.at[n], recv_sem=mix_recv.at[n],
                device_id={"seq": peer}, device_id_type=MESH,
            )
            copy.start()
            mix_copies.append(copy)

    pools = [pool_group(g) for g in range(pool_groups)]
    early = 2
    scores = [[] for _ in pools]
    for t in range(tiles):
        for copy in query_copies[3 * t : 3 * (t + 1)]:
            copy.wait()
        lanes = slice(t * half, (t + 1) * half)
        page_query[:, lanes] = jnp.dot(
            onehot[...], queries[:, :, lanes].reshape(requests, half),
            preferred_element_type=jnp.float32,
        ).astype(jnp.bfloat16)
        if t == 0:
            for g in range(early):
                pool_copy(g).wait()
                scores[g].append(pool_scores(pools[g], g, t))
    for g in range(pool_groups):
        if g >= early:
            pool_copy(g).wait()
        for t in range(len(scores[g]), tiles):
            scores[g].append(pool_scores(pools[g], g, t))
        if g:
            finish_pool(g - 1, pools[g - 1], scores[g - 1])
    finish_pool(pool_groups - 1, pools[-1], scores[-1])
    high = page_mix[...].astype(jnp.bfloat16)
    both[:pages, :] = high
    both[pages:, :] = (page_mix[...] - high.astype(jnp.float32)).astype(jnp.bfloat16)
    req_mix[...] = jnp.dot(onehot_t[...], both[...], preferred_element_type=jnp.float32)
    for b in range(n_tasks // SLOTS):
        prompt_copy(b).wait()
    made = prompt_group(0)
    ahead = (made, prompt_scores(made, 0))
    for n in range(1, len(takers) * halves):
        made = prompt_group(n)
        later = (made, prompt_scores(made, n))
        finish_prompt(n - 1, *ahead)
        ahead = later
    finish_prompt(len(takers) * halves - 1, *ahead)

    def kv_product(src, dst, sem):
        acc = None
        for c in range(steps):
            kv_copy(src, dst, sem, c).wait()
            term = jnp.dot(
                normed[:, c * chunk : (c + 1) * chunk],
                dst[c * chunk : (c + 1) * chunk, :],
                preferred_element_type=jnp.float32,
            )
            acc = term if acc is None else acc + term
        return acc

    key_new = kv_product(w_key, k_buf, k_sem)
    value_new = kv_product(w_value, v_buf, v_sem)
    for g in range(kv_heads):
        lanes = slice(g * hd, (g + 1) * hd)
        fresh[0, :, lanes] = rope_lanes(key_new[:, lanes], cos_all, sin_all).astype(jnp.bfloat16)
    self_weights = []
    for h in range(heads):
        g = h // group
        q = queries[me, :, h * hd : (h + 1) * hd].astype(jnp.float32)
        k = fresh[0, :, g * hd : (g + 1) * hd].astype(jnp.float32)
        raw = jnp.sum(q * k, axis=1, keepdims=True)
        self_weights.append(jnp.exp(cap_limit * jnp.tanh(raw * (score_scale / cap_limit))))
    fresh[1] = value_new.astype(jnp.bfloat16)
    for i in range(2):
        fresh_rows[:, i, :] = fresh[i].astype(jnp.float32)
    fresh_out[...] = fresh_rows[...].astype(jnp.bfloat16)
    for copy in mix_copies:
        copy.wait()
    own = pl.ds(pl.multiple_of(me * rows, SLOTS), rows)
    totals = req_mix[own, q_width:]
    for k in range(3):
        totals += landed[k, :, q_width:].astype(jnp.float32)
    for h in range(heads):
        g = h // group
        lanes = slice(h * hd, (h + 1) * hd)
        mix = req_mix[own, lanes]
        for k in range(3):
            mix += landed[k, :, lanes].astype(jnp.float32)
        total = totals[:, h : h + 1] + self_weights[h]
        rounded = self_weights[h].astype(jnp.bfloat16).astype(jnp.float32)
        mix += rounded * fresh[1, :, g * hd : (g + 1) * hd].astype(jnp.float32)
        attended[:, lanes] = (mix / total).astype(jnp.bfloat16)

    is_inner = lax.rem(mine, 3) != 0
    onward = lax.rem(2 * mine + 1, 5)
    pieces = (slice(0, cut), slice(cut, cols))

    def project(k, piece):
        return jnp.dot(attended[...], w_buf[k, :, piece], preferred_element_type=jnp.float32)

    def part(i, k, piece, peer):
        return pltpu.make_async_remote_copy(
            src_ref=sent.at[k, :, piece], dst_ref=arrived.at[k, :, piece],
            send_sem=part_send.at[i], recv_sem=part_recv.at[i],
            device_id={"tensor": peer}, device_id_type=MESH,
        )

    handed = [part(0, 0, pieces[0], onward), part(1, 0, pieces[1], tensor_peers[0])]
    mirrored = [part(2 + i, 1, pieces[i], tensor_peers[1]) for i in range(2)]
    beside = part(4, 2, slice(0, cols), tensor_peers[2])
    for k in range(4):
        for i in range(2):
            w_copy(k, i).wait()

    def ship(k, piece, product, copy):
        sent[k, :, piece] = product.astype(jnp.bfloat16)
        copy.start()

    whole_piece = slice(0, cols)
    first = project(0, pieces[0])
    second = project(0, pieces[1])
    ship(0, pieces[0], first, handed[0])
    third = project(1, pieces[1])
    ship(0, pieces[1], second, handed[1])
    held[...] = project(1, pieces[0])
    ship(1, pieces[1], third, mirrored[1])

    @pl.when(jnp.logical_not(is_inner))
    def _():
        ship(1, pieces[0], held[...], mirrored[0])

    fourth = project(2, whole_piece)
    whole_sum[...] = project(3, whole_piece)
    ship(2, whole_piece, fourth, beside)
    @pl.when(is_inner)
    def _():
        handed[0].wait_recv()
        total = held[...] + arrived[0, :, pieces[0]].astype(jnp.float32)
        sent[1, :, pieces[0]] = total.astype(jnp.bfloat16)
        mirrored[0].start()

    beside.wait_recv()
    whole_sum[...] += arrived[2].astype(jnp.float32)
    handed[1].wait_recv()
    whole_sum[:, pieces[1]] += arrived[0, :, pieces[1]].astype(jnp.float32)

    @pl.when(jnp.logical_not(is_inner))
    def _():
        handed[0].wait_recv()
        whole_sum[:, pieces[0]] += arrived[0, :, pieces[0]].astype(jnp.float32)

    for copy in mirrored:
        copy.wait_recv()
    whole = whole_sum[...] + arrived[1].astype(jnp.float32)
    part_square = jnp.sum(whole * whole, axis=1, keepdims=True)
    row = lax.broadcasted_iota(jnp.int32, (rows, 128), 0)
    diagonal = row == lax.broadcasted_iota(jnp.int32, (rows, 128), 1)
    square[...] = jnp.sum(jnp.where(diagonal, part_square, 0.0), axis=0, keepdims=True)
    copies = []
    for k, peer in enumerate(tensor_peers):
        copy = pltpu.make_async_remote_copy(
            src_ref=square, dst_ref=squares.at[k],
            send_sem=square_send.at[k], recv_sem=square_recv.at[k],
            device_id={"tensor": peer}, device_id_type=MESH,
        )
        copy.start()
        copies.append(copy)
    scaled = whole * post_gain[...][None]
    start = pl.multiple_of(mine * cols, 128)
    residual = hidden[:, pl.ds(start, cols)].astype(jnp.float32)
    for copy in copies:
        copy.wait()
    total_square = square[...]
    for k in range(3):
        total_square += squares[k]
    column_square = jnp.sum(jnp.where(diagonal, total_square, 0.0), axis=1, keepdims=True)
    factor = lax.rsqrt(column_square / (cols * tensor) + 1e-06)
    out[...] = (residual + scaled * factor).astype(jnp.bfloat16)
    for copy in handed + mirrored + [beside]:
        copy.wait_send()


STEPS = 3


def place_kernel(layer_in, fresh_in, layer_out, fresh_out, sems):
    copies = [
        pltpu.make_async_copy(layer_in, layer_out, sems.at[0]),
        pltpu.make_async_copy(fresh_in, fresh_out, sems.at[1]),
    ]
    for copy in copies:
        copy.start()
    for copy in copies:
        copy.wait()


def body(
    seq, tensor, hidden, pre_gain, w_query, w_key, w_value, w_out, post_gain,
    cache_pool, prompt_cache, task_ids, cache_lengths, block_table,
):
    rows, depth = hidden.shape
    requests = task_ids.shape[0]
    pages, _, _, kv_width = cache_pool.shape
    n_tasks = prompt_cache.shape[0]
    q_width = w_query.shape[1]
    heads = q_width // HD
    cols = post_gain.shape[0]
    score_scale = float(D // H) ** (-0.5)
    half = HD // 2
    frequency = 10000.0 ** (-np.arange(half) / half)
    frequency = jnp.asarray(np.concatenate([frequency, frequency])[None], jnp.float32)
    vmem = pl.BlockSpec(memory_space=pltpu.VMEM)
    hbm = pl.BlockSpec(memory_space=pl.ANY)
    dma = pltpu.SemaphoreType.DMA
    bf16, f32, i32 = jnp.bfloat16, jnp.float32, jnp.int32
    packed_width = q_width + HD
    layer_out, fresh = pl.pallas_call(
        functools.partial(layer_kernel, seq, tensor, score_scale, HD, STEPS),
        out_shape=(
            pltpu.VMEM((rows, cols), bf16),
            pltpu.VMEM((rows, 2, kv_width), bf16),
        ),
        in_specs=[hbm] * 14,
        out_specs=(vmem, vmem),
        scratch_shapes=[
            pltpu.VMEM((1, requests), i32),
            pltpu.SMEM((requests,), i32),
            pltpu.VMEM((1, requests), i32),
            pltpu.VMEM((block_table.shape[1], requests), i32),
            pltpu.VMEM((rows, depth), bf16),
            pltpu.VMEM((depth,), f32),
            pltpu.VMEM((1, HD), f32),
            pltpu.VMEM((cols,), f32),
            pltpu.VMEM((rows, depth), bf16),
            pltpu.VMEM((seq, rows, q_width), bf16),
            pltpu.VMEM((depth, q_width), bf16),
            pltpu.VMEM((depth, kv_width), bf16),
            pltpu.VMEM((depth, kv_width), bf16),
            pltpu.VMEM((tensor, w_out.shape[0], cols), bf16),
            pltpu.VMEM(cache_pool.shape, bf16),
            pltpu.VMEM(prompt_cache.shape, bf16),
            pltpu.VMEM((pages, requests), bf16),
            pltpu.VMEM((requests, 2 * pages), bf16),
            pltpu.VMEM((pages, TOKENS), f32),
            pltpu.VMEM((requests, TOKENS), f32),
            pltpu.VMEM((pages, q_width), bf16),
            pltpu.VMEM((4, heads * SLOTS, kv_width), bf16),
            pltpu.VMEM((pages, packed_width), f32),
            pltpu.VMEM((2 * pages, packed_width), bf16),
            pltpu.VMEM((requests, packed_width), f32),
            pltpu.VMEM((3, rows, packed_width), bf16),
            pltpu.VMEM((3, rows, packed_width), bf16),
            pltpu.VMEM((2, rows, kv_width), bf16),
            pltpu.VMEM((rows, 2, kv_width), f32),
            pltpu.VMEM((rows, q_width), bf16),
            pltpu.VMEM((3, rows, cols), bf16),
            pltpu.VMEM((3, rows, cols), bf16),
            pltpu.VMEM((rows, cols // 256 * 128), f32),
            pltpu.VMEM((rows, cols), f32),
            pltpu.VMEM((1, 128), f32),
            pltpu.VMEM((3, 1, 128), f32),
            dma((8,)),
            dma((2 * STEPS,)),
            dma((STEPS,)),
            dma((STEPS,)),
            dma((2 * tensor,)),
            dma((pages // SLOTS,)),
            dma((n_tasks // SLOTS,)),
            dma((6,)),
            dma((6,)),
            dma((6,)),
            dma((6,)),
            dma((5,)),
            dma((5,)),
            dma((3,)),
            dma((3,)),
        ],
        compiler_params=pltpu.CompilerParams(
            collective_id=0, has_side_effects=True, vmem_limit_bytes=VMEM_BYTES
        ),
    )(
        cache_lengths.reshape(1, -1), task_ids, task_ids.reshape(1, -1), block_table.T,
        hidden, pre_gain, frequency, post_gain,
        w_query, w_key, w_value, w_out, cache_pool, prompt_cache,
    )
    return pl.pallas_call(
        place_kernel,
        out_shape=(
            jax.ShapeDtypeStruct((rows, cols), bf16),
            jax.ShapeDtypeStruct((rows, 2, kv_width), bf16),
        ),
        in_specs=[vmem, vmem],
        out_specs=(hbm, hbm),
        scratch_shapes=[dma((2,))],
        compiler_params=pltpu.CompilerParams(vmem_limit_bytes=1024 * 1024),
    )(layer_out, fresh)


def fits(seq, tensor, arrays):
    hidden, w_query, w_key, post_gain = arrays[0], arrays[2], arrays[3], arrays[6]
    pool, prompts, tasks = arrays[7], arrays[8], arrays[9]
    return (
        seq == 4
        and tensor == 4
        and hidden.shape[0] == 2 * SLOTS
        and hidden.shape[1] % (STEPS * 256) == 0
        and w_query.shape[1] == 8 * HD
        and w_key.shape[1] == 4 * HD
        and post_gain.shape[0] % 128 == 0
        and pool.shape[0] == 64
        and pool.shape[2] == TOKENS
        and prompts.shape[0] % SLOTS == 0
        and prompts.shape[2] == TOKENS // 2
        and tasks.shape[0] == 128
    )


def solution(mesh):
    seq, tensor = mesh.shape["seq"], mesh.shape["tensor"]

    def chosen(*arrays):
        if not fits(seq, tensor, arrays):
            return plain_body(*arrays)
        return body(seq, tensor, *arrays)

    return jax.shard_map(
        chosen,
        mesh=mesh,
        in_specs=(
            P(("groups", "seq"), None),
            P(),
            P(None, "tensor"),
            P(None, "tensor"),
            P(None, "tensor"),
            P("tensor", None),
            P("tensor"),
            P(("groups", "seq"), None, None, "tensor"),
            P("seq", None, None, "tensor"),
            P("groups"),
            P("groups"),
            P("groups", None),
        ),
        out_specs=(P(("groups", "seq"), "tensor"), P(("groups", "seq"), None, "tensor")),
        check_vma=False,
    )
```

```python
import jax
import jax.numpy as jnp
from jax import lax
from jax.experimental import pallas as pl
from jax.experimental.pallas import tpu as pltpu
from jax.sharding import PartitionSpec as P
import functools
import numpy as np

D = 4608
H = 32
HD = 128


cap_limit = 50.0


def rms_scale(values, gain):
    mean_square = jnp.mean(values * values, axis=-1, keepdims=True)
    return values * lax.rsqrt(mean_square + 1e-06) * gain


def rotate(values, position):
    half_dim = values.shape[-1] // 2
    frequency = 10000.0 ** (-jnp.arange(half_dim, dtype=jnp.float32) / half_dim)
    angles = position.astype(jnp.float32)[:, None] * frequency[None, :]
    cosine = jnp.cos(angles)[:, None, :]
    sines = jnp.sin(angles)[:, None, :]
    first_half = values[..., :half_dim]
    second_half = values[..., half_dim:]
    return jnp.concatenate(
        [first_half * cosine - second_half * sines, second_half * cosine + first_half * sines],
        axis=-1,
    )


def capped(raw_score, score_scale):
    return cap_limit * jnp.tanh(raw_score * score_scale / cap_limit)


def attend(query_block, block, live_mask, score_scale):
    count = block.shape[0]
    length = block.shape[2]
    kv_heads = query_block.shape[1]
    head_dim = query_block.shape[3]
    block_keys = block[:, 0].reshape(count, length, kv_heads, head_dim)
    block_values = block[:, 1].reshape(count, length, kv_heads, head_dim)
    raw_score = jnp.einsum(
        "nkgd,ntkd->nkgt", query_block, block_keys, preferred_element_type=jnp.float32
    )
    weight = jnp.where(live_mask[:, None, None, :], jnp.exp(capped(raw_score, score_scale)), 0.0)
    totals = jnp.sum(weight, axis=-1).reshape(count, -1)
    mixtures = jnp.einsum(
        "nkgt,ntkd->nkgd",
        weight.astype(jnp.bfloat16),
        block_values,
        preferred_element_type=jnp.float32,
    )
    return (totals, mixtures.reshape(count, -1))


def plain_body(
    hidden,
    pre_gain,
    w_query,
    w_key,
    w_value,
    w_out,
    post_gain,
    cache_pool,
    prompt_cache,
    task_ids,
    cache_lengths,
    block_table,
):
    seq_index = lax.axis_index("seq")
    tensor_index = lax.axis_index("tensor")
    own_rows = hidden.shape[0]
    requests = task_ids.shape[0]
    pages_dev = cache_pool.shape[0]
    block_len = cache_pool.shape[2]
    kv_width = cache_pool.shape[3]
    head_dim = HD
    kv_heads = kv_width // head_dim
    query_heads = w_query.shape[1] // head_dim
    group_size = query_heads // kv_heads
    prompt_len = prompt_cache.shape[2]
    tasks_dev = prompt_cache.shape[0]
    score_scale = float(D // H) ** (-0.5)
    first_row = seq_index * own_rows
    own_lengths = lax.dynamic_slice_in_dim(cache_lengths, first_row, own_rows)
    normed = rms_scale(hidden.astype(jnp.float32), pre_gain).astype(jnp.bfloat16)
    position = prompt_len + own_lengths
    query_rows = rotate(
        jnp.dot(normed, w_query, preferred_element_type=jnp.float32).reshape(
            own_rows, query_heads, head_dim
        ),
        position,
    ).astype(jnp.bfloat16)
    key_new = rotate(
        jnp.dot(normed, w_key, preferred_element_type=jnp.float32).reshape(
            own_rows, kv_heads, head_dim
        ),
        position,
    ).astype(jnp.bfloat16)
    value_new = jnp.dot(normed, w_value, preferred_element_type=jnp.float32).astype(jnp.bfloat16)
    fresh_cache = jnp.stack([key_new.reshape(own_rows, kv_width), value_new], axis=1)
    queries = lax.all_gather(
        query_rows.reshape(own_rows, query_heads * head_dim), "seq", axis=0, tiled=True
    )
    page_ids = seq_index * pages_dev + jnp.arange(pages_dev)
    flat_table = block_table.reshape(-1)
    max_blocks = block_table.shape[1]
    matches = flat_table[None, :] == page_ids[:, None]
    entry_index = jnp.arange(flat_table.shape[0])
    page_used = jnp.any(matches, axis=1)
    found_entry = jnp.sum(jnp.where(matches, entry_index[None, :], 0), axis=1)
    page_owner = found_entry // max_blocks
    block_number = found_entry % max_blocks
    owner_hot = (page_owner[:, None] == jnp.arange(requests)[None, :]) & page_used[:, None]
    owner_length = jnp.sum(jnp.where(owner_hot, cache_lengths[None, :], 0), axis=1)
    valid_count = jnp.clip(owner_length - block_number * block_len, 0, block_len)
    page_query = jnp.dot(
        owner_hot.astype(jnp.bfloat16), queries, preferred_element_type=jnp.float32
    ).astype(jnp.bfloat16)
    page_query = page_query.reshape(pages_dev, kv_heads, group_size, head_dim)
    page_live = jnp.arange(block_len)[None, :] < valid_count[:, None]
    page_totals, page_mixtures = attend(page_query, cache_pool, page_live, score_scale)
    spread_hot = owner_hot.astype(jnp.float32).T
    totals = jnp.dot(spread_hot, page_totals, precision=lax.Precision.HIGHEST)
    mixtures = jnp.dot(spread_hot, page_mixtures, precision=lax.Precision.HIGHEST)
    local_task = task_ids - seq_index * tasks_dev
    is_owned = (local_task >= 0) & (local_task < tasks_dev)
    task_rows = prompt_cache[jnp.clip(local_task, 0, tasks_dev - 1)]
    all_query = queries.reshape(requests, kv_heads, group_size, head_dim)
    owned_live = jnp.broadcast_to(is_owned[:, None], (requests, prompt_len))
    prompt_totals, prompt_mixtures = attend(all_query, task_rows, owned_live, score_scale)
    totals = totals + prompt_totals
    mixtures = mixtures + prompt_mixtures
    totals, mixtures = (
        lax.psum_scatter(
            totals.astype(jnp.bfloat16), "seq", scatter_dimension=0, tiled=True
        ).astype(jnp.float32),
        lax.psum_scatter(
            mixtures.astype(jnp.bfloat16), "seq", scatter_dimension=0, tiled=True
        ).astype(jnp.float32),
    )
    own_query = query_rows.reshape(own_rows, kv_heads, group_size, head_dim)
    self_raw = jnp.sum(
        own_query.astype(jnp.float32) * key_new[:, :, None, :].astype(jnp.float32), axis=-1
    )
    self_weight = jnp.exp(capped(self_raw, score_scale))
    rounded = lax.optimization_barrier(self_weight.astype(jnp.bfloat16)).astype(jnp.float32)
    totals = totals + self_weight.reshape(own_rows, -1)
    self_mix = rounded[..., None] * value_new.reshape(own_rows, kv_heads, 1, head_dim).astype(
        jnp.float32
    )
    mixtures = mixtures + self_mix.reshape(own_rows, -1)
    attended = (mixtures.reshape(own_rows, query_heads, head_dim) / totals[..., None]).astype(
        jnp.bfloat16
    )
    projected = jnp.dot(
        attended.reshape(own_rows, query_heads * head_dim),
        w_out,
        preferred_element_type=jnp.float32,
    )
    cols_local = post_gain.shape[0]
    col_start = tensor_index * cols_local
    residual = lax.dynamic_slice_in_dim(hidden, col_start, cols_local, 1).astype(jnp.float32)
    whole_sum = lax.psum(projected.astype(jnp.bfloat16), "tensor").astype(jnp.float32)
    mean_square = jnp.mean(whole_sum * whole_sum, axis=1, keepdims=True)
    scaled = lax.dynamic_slice_in_dim(whole_sum, col_start, cols_local, 1) * lax.rsqrt(
        mean_square + 1e-06
    )
    layer_out = (residual + scaled * post_gain).astype(jnp.bfloat16)
    return (layer_out, fresh_cache)


MESH = pl.DeviceIdType.MESH
VMEM_BYTES = 62 * 1024 * 1024


def rope_lanes(x, cosine, sines):
    return x * cosine + pltpu.roll(x, x.shape[-1] // 2, 1) * sines


SLOTS = 16
TOKENS = 128


def stacked(x, count):
    return jnp.concatenate([x] * count, axis=0)


def slot_unit(per):
    return lax.broadcasted_iota(jnp.int32, (SLOTS, TOKENS), 0) // per


def tile_scores(sizes, t, qwide, keys, values, pairs, per, live):
    heads, kv_heads, hd, score_scale = sizes
    tile_heads = heads * 256 // (kv_heads * hd)
    rows = tile_heads * SLOTS
    unit = stacked(slot_unit(per), tile_heads)
    across = lax.broadcasted_iota(jnp.int32, (TOKENS, rows), 1) % SLOTS // per
    q = qwide[t * rows : (t + 1) * rows, t * 256 : (t + 1) * 256]
    held, streamed = None, None
    for pair in range(pairs):
        two = (keys(pair, t), q) if pair % 2 == 0 else (q, keys(pair, t))
        raw = lax.dot_general(
            *two, (((1,), (1,)), ((), ())), preferred_element_type=jnp.float32
        )
        for u in range(2):
            if pair % 2 == 0:
                part = raw[u * TOKENS : (u + 1) * TOKENS]
                streamed = part if streamed is None else jnp.where(
                    across == 2 * pair + u, part, streamed
                )
            else:
                part = raw[:, u * TOKENS : (u + 1) * TOKENS]
                held = part if held is None else jnp.where(unit == 2 * pair + u, part, held)
    return jnp.where(unit // 2 % 2 == 0, streamed.T, held)


def tile_mixes(sizes, chosen, t, qwide, keys, values, pairs, per, live):
    heads, kv_heads, hd, score_scale = sizes
    tile_heads = heads * 256 // (kv_heads * hd)
    weight = jnp.exp(cap_limit * jnp.tanh(chosen * (score_scale / cap_limit)))
    weight = jnp.where(stacked(live, tile_heads) > 0, weight, 0.0)
    total = jnp.sum(weight, axis=1, keepdims=True)
    narrow = weight.astype(jnp.bfloat16)
    acc = None
    for pair in range(pairs):
        pieces = []
        for u in range(2):
            keep = (slot_unit(per) == 2 * pair + u).astype(jnp.float32).astype(jnp.bfloat16)
            pieces.append(narrow * stacked(keep, tile_heads))
        term = jnp.dot(
            jnp.concatenate(pieces, axis=1), values(pair, t), preferred_element_type=jnp.float32
        )
        acc = term if acc is None else acc + term
    mixes, totals = [], []
    for i in range(tile_heads):
        span = slice(i * SLOTS, (i + 1) * SLOTS)
        kv = i // (heads // kv_heads)
        mixes.append(acc[span, kv * hd : (kv + 1) * hd])
        totals.append(total[span])
    return mixes, totals


def group_mixes(sizes, scores, group):
    heads, hd = sizes[0], sizes[2]
    mixes, totals = [], []
    for t, chosen in enumerate(scores):
        more = tile_mixes(sizes, chosen, t, *group)
        mixes += more[0]
        totals += more[1]
    lane = lax.broadcasted_iota(jnp.int32, (SLOTS, hd), 1)
    packed_total = jnp.zeros((SLOTS, hd), jnp.float32)
    for h in range(heads):
        packed_total = jnp.where(lane == h, totals[h], packed_total)
    return mixes + [packed_total]


def layer_kernel(
    seq, tensor, score_scale, hd, steps,
    lengths_in, tasks_in, tasks_row_in, table_in, hidden_in, pre_gain_in, frequency_in, post_gain_in,
    w_query, w_key, w_value, w_out, pool, prompts,
    out, fresh_out,
    lengths, tasks, tasks_row, table, hidden, pre_gain, frequency, post_gain,
    normed, queries, q_buf, k_buf, v_buf, w_buf, pool_buf, prompt_buf,
    onehot, onehot_t, valid, owned, page_query, qwide, page_mix, both, req_mix, packed, landed,
    fresh, fresh_rows, attended, sent, arrived, held, whole_sum, square, squares,
    small_sem, q_sem, k_sem, v_sem, w_sem, pool_sem, prompt_sem,
    query_send, query_recv, mix_send, mix_recv, part_send, part_recv, square_send, square_recv,
):
    me = lax.axis_index("seq")
    mine = lax.axis_index("tensor")
    rows, depth = hidden.shape
    cols = out.shape[1]
    requests = lengths.shape[1]
    q_width = q_buf.shape[1]
    kv_width = k_buf.shape[1]
    heads, kv_heads = q_width // hd, kv_width // hd
    group = heads // kv_heads
    pages, _, block_len, _ = pool.shape
    n_tasks, _, prompt_len, _ = prompts.shape
    max_blocks = table.shape[0]
    half = q_width // 2
    chunk = depth // steps
    cut = cols // 256 * 128

    smalls = []
    for i, (src, dst) in enumerate((
        (hidden_in, hidden), (pre_gain_in, pre_gain), (frequency_in, frequency),
        (lengths_in, lengths), (tasks_in, tasks), (tasks_row_in, tasks_row),
        (table_in, table), (post_gain_in, post_gain),
    )):
        smalls.append(pltpu.make_async_copy(src, dst, small_sem.at[i]))

    def q_copy(n, c):
        span, lanes = pl.ds(c * chunk, chunk), pl.ds(n * half, half)
        return pltpu.make_async_copy(
            w_query.at[span, lanes], q_buf.at[span, lanes], q_sem.at[n * steps + c]
        )

    def kv_copy(src, dst, sem, c):
        span = pl.ds(c * chunk, chunk)
        return pltpu.make_async_copy(src.at[span], dst.at[span], sem.at[c])

    def pool_copy(b):
        span = pl.ds(b * SLOTS, SLOTS)
        return pltpu.make_async_copy(pool.at[span], pool_buf.at[span], pool_sem.at[b])

    def prompt_copy(b):
        span = pl.ds(b * SLOTS, SLOTS)
        return pltpu.make_async_copy(prompts.at[span], prompt_buf.at[span], prompt_sem.at[b])

    def partners(i):
        return [3 - i, lax.rem(i + 2, 4), i + 1 - 2 * lax.rem(i, 2)]

    seq_peers = partners(me)
    tensor_peers = [lax.rem(mine + 2, 4), 3 - mine, mine + 1 - 2 * lax.rem(mine, 2)]

    w_rows = w_out.shape[0] // 2

    def w_copy(k, i):
        column = tensor_peers[k] if k < 3 else mine
        start = pl.multiple_of(column * cols, 128)
        span = pl.ds(i * w_rows, w_rows)
        return pltpu.make_async_copy(
            w_out.at[span, pl.ds(start, cols)], w_buf.at[k, span], w_sem.at[2 * k + i]
        )

    for copy in smalls:
        copy.start()

    def start_all(count, start_one):
        def one(i, carry):
            start_one(i)
            return carry

        lax.fori_loop(0, count, one, 0)

    for n in range(2):
        start_all(steps, lambda c, n=n: q_copy(n, c).start())
    start_all(pages // SLOTS, lambda b: pool_copy(b).start())
    start_all(n_tasks // SLOTS, lambda b: prompt_copy(b).start())
    start_all(steps, lambda c: kv_copy(w_key, k_buf, k_sem, c).start())
    start_all(steps, lambda c: kv_copy(w_value, v_buf, v_sem, c).start())
    for k in range(4):
        start_all(2, lambda i, k=k: w_copy(k, i).start())

    barrier = pltpu.get_barrier_semaphore()
    for peer in seq_peers:
        pl.semaphore_signal(barrier, inc=1, device_id={"seq": peer}, device_id_type=MESH)
    for peer in tensor_peers:
        pl.semaphore_signal(barrier, inc=1, device_id={"tensor": peer}, device_id_type=MESH)

    qwide[...] = jnp.zeros_like(qwide)
    for copy in smalls:
        copy.wait()
    x = hidden[...].astype(jnp.float32)
    mean_square = jnp.mean(x * x, axis=-1, keepdims=True)
    normed[...] = (x * lax.rsqrt(mean_square + 1e-06) * pre_gain[...][None]).astype(jnp.bfloat16)

    row = lax.broadcasted_iota(jnp.int32, (rows, requests), 0)
    column = lax.broadcasted_iota(jnp.int32, (rows, requests), 1)
    own_length = jnp.sum(
        jnp.where(column == me * rows + row, lengths[...].astype(jnp.float32), 0.0),
        axis=1, keepdims=True,
    )
    angles = (own_length + prompt_len) * frequency[...]
    lane = lax.broadcasted_iota(jnp.int32, (rows, hd), 1)
    cos_all = jnp.cos(angles)
    sin_all = jnp.sin(angles)
    sin_all = jnp.where(lane < hd // 2, -sin_all, sin_all)

    query_copies = []
    for n in range(2):
        lanes = slice(n * half, (n + 1) * half)
        acc = None
        for c in range(steps):
            q_copy(n, c).wait()
            term = jnp.dot(
                normed[:, c * chunk : (c + 1) * chunk],
                q_buf[c * chunk : (c + 1) * chunk, lanes],
                preferred_element_type=jnp.float32,
            )
            acc = term if acc is None else acc + term
        turned = jnp.concatenate(
            [
                rope_lanes(acc[:, i * hd : (i + 1) * hd], cos_all, sin_all)
                for i in range(half // hd)
            ],
            axis=1,
        ).astype(jnp.bfloat16)
        queries[pl.ds(me, 1), :, lanes] = turned[None]
        if n == 0:
            pl.semaphore_wait(barrier, 6)
        for k, peer in enumerate(seq_peers):
            where = queries.at[me, :, pl.ds(n * half, half)]
            copy = pltpu.make_async_remote_copy(
                src_ref=where, dst_ref=where,
                send_sem=query_send.at[n * 3 + k], recv_sem=query_recv.at[n * 3 + k],
                device_id={"seq": peer}, device_id_type=MESH,
            )
            copy.start()
            query_copies.append(copy)

    page_id = me * pages + lax.broadcasted_iota(jnp.int32, (pages, requests), 0)

    def match_one(j, carry):
        hot, count = carry
        hit = jnp.broadcast_to(table[pl.ds(j, 1), :], (pages, requests)) == page_id
        tokens = jnp.broadcast_to(
            jnp.clip(lengths[...] - j * block_len, 0, block_len), (pages, requests)
        )
        return jnp.where(hit, 1.0, hot), jnp.where(hit, tokens.astype(jnp.float32), count)

    zeros = jnp.zeros((pages, requests), jnp.float32)
    hot, count = lax.fori_loop(0, max_blocks, match_one, (zeros, zeros))
    onehot[...] = hot.astype(jnp.bfloat16)
    turned = hot.T.astype(jnp.bfloat16)
    onehot_t[...] = jnp.concatenate([turned, turned], axis=1)
    valid[...] = jnp.broadcast_to(jnp.sum(count, axis=1, keepdims=True), valid.shape)
    line = lax.broadcasted_iota(jnp.int32, (requests, requests), 0)
    across = lax.broadcasted_iota(jnp.int32, (requests, requests), 1)
    local = tasks_row[...] - me * n_tasks
    is_owned = jnp.where((local >= 0) & (local < n_tasks), 1.0, 0.0)
    owned[...] = jnp.broadcast_to(
        jnp.sum(jnp.where(line == across, is_owned, 0.0), axis=1, keepdims=True), owned.shape
    )

    sizes = (heads, kv_heads, hd, score_scale)
    tiles = kv_width // 256
    tile_heads = heads // tiles
    token = lax.broadcasted_iota(jnp.int32, (SLOTS, TOKENS), 1)
    per = TOKENS // prompt_len
    slot_of = lax.broadcasted_iota(jnp.int32, (SLOTS, TOKENS), 0)
    fits = token // prompt_len == slot_of % per
    pool_groups = pages // SLOTS
    halves = rows // SLOTS
    takers = seq_peers + [me]

    def widen(slot, t, source):
        for h in range(t * tile_heads, (t + 1) * tile_heads):
            kv = h // group
            qwide[slot, h * SLOTS : (h + 1) * SLOTS, kv * hd : (kv + 1) * hd] = source(
                slice(h * hd, (h + 1) * hd)
            )

    def pool_group(g):
        start = g * SLOTS

        def load(which):
            def one(pair, t):
                first = start + 2 * pair
                return pool_buf[first : first + 2, which, :, t * 256 : (t + 1) * 256].reshape(
                    2 * block_len, 256
                )

            return one

        live = jnp.where(token.astype(jnp.float32) < valid[start : start + SLOTS, :], 1.0, 0.0)
        return (qwide.at[g % 4], load(0), load(1), SLOTS // 2, 1, live)

    def pool_scores(made, g, t):
        widen(g % 4, t, lambda lanes: page_query[g * SLOTS : (g + 1) * SLOTS, lanes])
        return tile_scores(sizes, t, *made)

    def prompt_group(n):
        peer, s = takers[n // halves], n % halves
        first = peer * rows + s * SLOTS
        places = [
            jnp.clip(tasks[first + i] - me * n_tasks, 0, n_tasks - 1) for i in range(SLOTS)
        ]

        def load(which):
            def one(pair, t):
                return jnp.concatenate(
                    [
                        prompt_buf[place, which, :, t * 256 : (t + 1) * 256]
                        for place in places[pair * 2 * per : (pair + 1) * 2 * per]
                    ],
                    axis=0,
                )

            return one

        start = pl.multiple_of(first, SLOTS)
        live = jnp.where(fits, owned[pl.ds(start, SLOTS), :], 0.0)
        return (qwide.at[n % 4], load(0), load(1), SLOTS // (2 * per), per, live)

    def prompt_scores(made, n):
        peer, s = takers[n // halves], n % halves
        scores = []
        for t in range(tiles):
            widen(n % 4, t, lambda lanes: queries[peer, s * SLOTS : (s + 1) * SLOTS, lanes])
            scores.append(tile_scores(sizes, t, *made))
        return scores

    def finish_pool(g, made, scores):
        for i, piece in enumerate(group_mixes(sizes, scores, made)):
            page_mix[g * SLOTS : (g + 1) * SLOTS, i * hd : (i + 1) * hd] = piece

    mix_copies = []

    def finish_prompt(n, made, scores):
        k, s = n // halves, n % halves
        peer = takers[k]
        span = slice(s * SLOTS, (s + 1) * SLOTS)
        start = pl.multiple_of(peer * rows + s * SLOTS, SLOTS)
        for i, piece in enumerate(group_mixes(sizes, scores, made)):
            lanes = slice(i * hd, (i + 1) * hd)
            sums = req_mix[pl.ds(start, SLOTS), lanes] + piece
            if k < 3:
                packed[k, span, lanes] = sums.astype(jnp.bfloat16)
            else:
                req_mix[pl.ds(start, SLOTS), lanes] = sums
        if k < 3:
            copy = pltpu.make_async_remote_copy(
                src_ref=packed.at[k, span], dst_ref=landed.at[k, span],
                send_sem=mix_send.at[n], recv_sem=mix_recv.at[n],
                device_id={"seq": peer}, device_id_type=MESH,
            )
            copy.start()
            mix_copies.append(copy)

    pools = [pool_group(g) for g in range(pool_groups)]
    early = 2
    scores = [[] for _ in pools]
    for t in range(tiles):
        for copy in query_copies[3 * t : 3 * (t + 1)]:
            copy.wait()
        lanes = slice(t * half, (t + 1) * half)
        page_query[:, lanes] = jnp.dot(
            onehot[...], queries[:, :, lanes].reshape(requests, half),
            preferred_element_type=jnp.float32,
        ).astype(jnp.bfloat16)
        if t == 0:
            for g in range(early):
                pool_copy(g).wait()
                scores[g].append(pool_scores(pools[g], g, t))
    for g in range(pool_groups):
        if g >= early:
            pool_copy(g).wait()
        for t in range(len(scores[g]), tiles):
            scores[g].append(pool_scores(pools[g], g, t))
        if g:
            finish_pool(g - 1, pools[g - 1], scores[g - 1])
    finish_pool(pool_groups - 1, pools[-1], scores[-1])
    high = page_mix[...].astype(jnp.bfloat16)
    both[:pages, :] = high
    both[pages:, :] = (page_mix[...] - high.astype(jnp.float32)).astype(jnp.bfloat16)
    req_mix[...] = jnp.dot(onehot_t[...], both[...], preferred_element_type=jnp.float32)
    for b in range(n_tasks // SLOTS):
        prompt_copy(b).wait()
    made = prompt_group(0)
    ahead = (made, prompt_scores(made, 0))
    for n in range(1, len(takers) * halves):
        made = prompt_group(n)
        later = (made, prompt_scores(made, n))
        finish_prompt(n - 1, *ahead)
        ahead = later
    finish_prompt(len(takers) * halves - 1, *ahead)

    def kv_product(src, dst, sem):
        acc = None
        for c in range(steps):
            kv_copy(src, dst, sem, c).wait()
            term = jnp.dot(
                normed[:, c * chunk : (c + 1) * chunk],
                dst[c * chunk : (c + 1) * chunk, :],
                preferred_element_type=jnp.float32,
            )
            acc = term if acc is None else acc + term
        return acc

    key_new = kv_product(w_key, k_buf, k_sem)
    value_new = kv_product(w_value, v_buf, v_sem)
    for g in range(kv_heads):
        lanes = slice(g * hd, (g + 1) * hd)
        fresh[0, :, lanes] = rope_lanes(key_new[:, lanes], cos_all, sin_all).astype(jnp.bfloat16)
    self_weights = []
    for h in range(heads):
        g = h // group
        q = queries[me, :, h * hd : (h + 1) * hd].astype(jnp.float32)
        k = fresh[0, :, g * hd : (g + 1) * hd].astype(jnp.float32)
        raw = jnp.sum(q * k, axis=1, keepdims=True)
        self_weights.append(jnp.exp(cap_limit * jnp.tanh(raw * (score_scale / cap_limit))))
    fresh[1] = value_new.astype(jnp.bfloat16)
    for i in range(2):
        fresh_rows[:, i, :] = fresh[i].astype(jnp.float32)
    fresh_out[...] = fresh_rows[...].astype(jnp.bfloat16)
    for copy in mix_copies:
        copy.wait()
    own = pl.ds(pl.multiple_of(me * rows, SLOTS), rows)
    totals = req_mix[own, q_width:]
    for k in range(3):
        totals += landed[k, :, q_width:].astype(jnp.float32)
    for h in range(heads):
        g = h // group
        lanes = slice(h * hd, (h + 1) * hd)
        mix = req_mix[own, lanes]
        for k in range(3):
            mix += landed[k, :, lanes].astype(jnp.float32)
        total = totals[:, h : h + 1] + self_weights[h]
        rounded = self_weights[h].astype(jnp.bfloat16).astype(jnp.float32)
        mix += rounded * fresh[1, :, g * hd : (g + 1) * hd].astype(jnp.float32)
        attended[:, lanes] = (mix / total).astype(jnp.bfloat16)

    is_inner = lax.rem(mine, 3) != 0
    onward = lax.rem(2 * mine + 1, 5)
    pieces = (slice(0, cut), slice(cut, cols))

    def project(k, piece):
        return jnp.dot(attended[...], w_buf[k, :, piece], preferred_element_type=jnp.float32)

    def part(i, k, piece, peer):
        return pltpu.make_async_remote_copy(
            src_ref=sent.at[k, :, piece], dst_ref=arrived.at[k, :, piece],
            send_sem=part_send.at[i], recv_sem=part_recv.at[i],
            device_id={"tensor": peer}, device_id_type=MESH,
        )

    handed = [part(0, 0, pieces[0], onward), part(1, 0, pieces[1], tensor_peers[0])]
    mirrored = [part(2 + i, 1, pieces[i], tensor_peers[1]) for i in range(2)]
    beside = part(4, 2, slice(0, cols), tensor_peers[2])
    for k in range(4):
        for i in range(2):
            w_copy(k, i).wait()

    def ship(k, piece, product, copy):
        sent[k, :, piece] = product.astype(jnp.bfloat16)
        copy.start()

    whole_piece = slice(0, cols)
    first = project(0, pieces[0])
    second = project(0, pieces[1])
    ship(0, pieces[0], first, handed[0])
    third = project(1, pieces[1])
    ship(0, pieces[1], second, handed[1])
    held[...] = project(1, pieces[0])
    ship(1, pieces[1], third, mirrored[1])

    @pl.when(jnp.logical_not(is_inner))
    def _():
        ship(1, pieces[0], held[...], mirrored[0])

    fourth = project(2, whole_piece)
    whole_sum[...] = project(3, whole_piece)
    ship(2, whole_piece, fourth, beside)
    @pl.when(is_inner)
    def _():
        handed[0].wait_recv()
        total = held[...] + arrived[0, :, pieces[0]].astype(jnp.float32)
        sent[1, :, pieces[0]] = total.astype(jnp.bfloat16)
        mirrored[0].start()

    beside.wait_recv()
    whole_sum[...] += arrived[2].astype(jnp.float32)
    handed[1].wait_recv()
    whole_sum[:, pieces[1]] += arrived[0, :, pieces[1]].astype(jnp.float32)

    @pl.when(jnp.logical_not(is_inner))
    def _():
        handed[0].wait_recv()
        whole_sum[:, pieces[0]] += arrived[0, :, pieces[0]].astype(jnp.float32)

    for copy in mirrored:
        copy.wait_recv()
    whole = whole_sum[...] + arrived[1].astype(jnp.float32)
    part_square = jnp.sum(whole * whole, axis=1, keepdims=True)
    row = lax.broadcasted_iota(jnp.int32, (rows, 128), 0)
    diagonal = row == lax.broadcasted_iota(jnp.int32, (rows, 128), 1)
    square[...] = jnp.sum(jnp.where(diagonal, part_square, 0.0), axis=0, keepdims=True)
    copies = []
    for k, peer in enumerate(tensor_peers):
        copy = pltpu.make_async_remote_copy(
            src_ref=square, dst_ref=squares.at[k],
            send_sem=square_send.at[k], recv_sem=square_recv.at[k],
            device_id={"tensor": peer}, device_id_type=MESH,
        )
        copy.start()
        copies.append(copy)
    scaled = whole * post_gain[...][None]
    start = pl.multiple_of(mine * cols, 128)
    residual = hidden[:, pl.ds(start, cols)].astype(jnp.float32)
    for copy in copies:
        copy.wait()
    total_square = square[...]
    for k in range(3):
        total_square += squares[k]
    column_square = jnp.sum(jnp.where(diagonal, total_square, 0.0), axis=1, keepdims=True)
    factor = lax.rsqrt(column_square / (cols * tensor) + 1e-06)
    out[...] = (residual + scaled * factor).astype(jnp.bfloat16)
    for copy in handed + mirrored + [beside]:
        copy.wait_send()


STEPS = 6


def place_kernel(layer_in, fresh_in, layer_out, fresh_out, sems):
    copies = [
        pltpu.make_async_copy(layer_in, layer_out, sems.at[0]),
        pltpu.make_async_copy(fresh_in, fresh_out, sems.at[1]),
    ]
    for copy in copies:
        copy.start()
    for copy in copies:
        copy.wait()


def body(
    seq, tensor, hidden, pre_gain, w_query, w_key, w_value, w_out, post_gain,
    cache_pool, prompt_cache, task_ids, cache_lengths, block_table,
):
    rows, depth = hidden.shape
    requests = task_ids.shape[0]
    pages, _, _, kv_width = cache_pool.shape
    n_tasks = prompt_cache.shape[0]
    q_width = w_query.shape[1]
    heads = q_width // HD
    cols = post_gain.shape[0]
    score_scale = float(D // H) ** (-0.5)
    half = HD // 2
    frequency = 10000.0 ** (-np.arange(half) / half)
    frequency = jnp.asarray(np.concatenate([frequency, frequency])[None], jnp.float32)
    vmem = pl.BlockSpec(memory_space=pltpu.VMEM)
    hbm = pl.BlockSpec(memory_space=pl.ANY)
    dma = pltpu.SemaphoreType.DMA
    bf16, f32, i32 = jnp.bfloat16, jnp.float32, jnp.int32
    packed_width = q_width + HD
    layer_out, fresh = pl.pallas_call(
        functools.partial(layer_kernel, seq, tensor, score_scale, HD, STEPS),
        out_shape=(
            pltpu.VMEM((rows, cols), bf16),
            pltpu.VMEM((rows, 2, kv_width), bf16),
        ),
        in_specs=[hbm] * 14,
        out_specs=(vmem, vmem),
        scratch_shapes=[
            pltpu.VMEM((1, requests), i32),
            pltpu.SMEM((requests,), i32),
            pltpu.VMEM((1, requests), i32),
            pltpu.VMEM((block_table.shape[1], requests), i32),
            pltpu.VMEM((rows, depth), bf16),
            pltpu.VMEM((depth,), f32),
            pltpu.VMEM((1, HD), f32),
            pltpu.VMEM((cols,), f32),
            pltpu.VMEM((rows, depth), bf16),
            pltpu.VMEM((seq, rows, q_width), bf16),
            pltpu.VMEM((depth, q_width), bf16),
            pltpu.VMEM((depth, kv_width), bf16),
            pltpu.VMEM((depth, kv_width), bf16),
            pltpu.VMEM((tensor, w_out.shape[0], cols), bf16),
            pltpu.VMEM(cache_pool.shape, bf16),
            pltpu.VMEM(prompt_cache.shape, bf16),
            pltpu.VMEM((pages, requests), bf16),
            pltpu.VMEM((requests, 2 * pages), bf16),
            pltpu.VMEM((pages, TOKENS), f32),
            pltpu.VMEM((requests, TOKENS), f32),
            pltpu.VMEM((pages, q_width), bf16),
            pltpu.VMEM((4, heads * SLOTS, kv_width), bf16),
            pltpu.VMEM((pages, packed_width), f32),
            pltpu.VMEM((2 * pages, packed_width), bf16),
            pltpu.VMEM((requests, packed_width), f32),
            pltpu.VMEM((3, rows, packed_width), bf16),
            pltpu.VMEM((3, rows, packed_width), bf16),
            pltpu.VMEM((2, rows, kv_width), bf16),
            pltpu.VMEM((rows, 2, kv_width), f32),
            pltpu.VMEM((rows, q_width), bf16),
            pltpu.VMEM((3, rows, cols), bf16),
            pltpu.VMEM((3, rows, cols), bf16),
            pltpu.VMEM((rows, cols // 256 * 128), f32),
            pltpu.VMEM((rows, cols), f32),
            pltpu.VMEM((1, 128), f32),
            pltpu.VMEM((3, 1, 128), f32),
            dma((8,)),
            dma((2 * STEPS,)),
            dma((STEPS,)),
            dma((STEPS,)),
            dma((2 * tensor,)),
            dma((pages // SLOTS,)),
            dma((n_tasks // SLOTS,)),
            dma((6,)),
            dma((6,)),
            dma((6,)),
            dma((6,)),
            dma((5,)),
            dma((5,)),
            dma((3,)),
            dma((3,)),
        ],
        compiler_params=pltpu.CompilerParams(
            collective_id=0, has_side_effects=True, vmem_limit_bytes=VMEM_BYTES
        ),
    )(
        cache_lengths.reshape(1, -1), task_ids, task_ids.reshape(1, -1), block_table.T,
        hidden, pre_gain, frequency, post_gain,
        w_query, w_key, w_value, w_out, cache_pool, prompt_cache,
    )
    return pl.pallas_call(
        place_kernel,
        out_shape=(
            jax.ShapeDtypeStruct((rows, cols), bf16),
            jax.ShapeDtypeStruct((rows, 2, kv_width), bf16),
        ),
        in_specs=[vmem, vmem],
        out_specs=(hbm, hbm),
        scratch_shapes=[dma((2,))],
        compiler_params=pltpu.CompilerParams(vmem_limit_bytes=1024 * 1024),
    )(layer_out, fresh)


def fits(seq, tensor, arrays):
    hidden, w_query, w_key, post_gain = arrays[0], arrays[2], arrays[3], arrays[6]
    pool, prompts, tasks = arrays[7], arrays[8], arrays[9]
    return (
        seq == 4
        and tensor == 4
        and hidden.shape[0] == 2 * SLOTS
        and hidden.shape[1] % (STEPS * 256) == 0
        and w_query.shape[1] == 8 * HD
        and w_key.shape[1] == 4 * HD
        and post_gain.shape[0] % 128 == 0
        and pool.shape[0] == 64
        and pool.shape[2] == TOKENS
        and prompts.shape[0] % SLOTS == 0
        and prompts.shape[2] == TOKENS // 2
        and tasks.shape[0] == 128
    )


def solution(mesh):
    seq, tensor = mesh.shape["seq"], mesh.shape["tensor"]

    def chosen(*arrays):
        if not fits(seq, tensor, arrays):
            return plain_body(*arrays)
        return body(seq, tensor, *arrays)

    return jax.shard_map(
        chosen,
        mesh=mesh,
        in_specs=(
            P(("groups", "seq"), None),
            P(),
            P(None, "tensor"),
            P(None, "tensor"),
            P(None, "tensor"),
            P("tensor", None),
            P("tensor"),
            P(("groups", "seq"), None, None, "tensor"),
            P("seq", None, None, "tensor"),
            P("groups"),
            P("groups"),
            P("groups", None),
        ),
        out_specs=(P(("groups", "seq"), "tensor"), P(("groups", "seq"), None, "tensor")),
        check_vma=False,
    )
```
